128 devices in a mesh: hi: 4 (over y), lo: 32 (over x, z, core).
Axes of the slice: x: 4, y: 4, z: 4, core: 2. Of those that a mesh axis runs over, the one named last changes fastest.
Arguments:
- initial_state: float32 [2, 16777216], P(None, ('hi', 'lo')), may hold values from -60 to 60
- gate_angles: float32 [2, 3, 24], replicated, may hold values from -3.140625 to 3.140625
- damp_qubits: int32 [2, 4], replicated, may hold values from 0 to 16, as said below
- kraus_branch: int32 [2, 4], replicated, may hold values 0 or 1
- damping: float32 [2, 4], replicated, may hold values from 0.1 to 0.6
Outputs:
- final_state: float32 [2, 16777216], P(None, ('hi', 'lo'))
- branch_weights: float32 [2, 4], replicated
The draws below stay inside these ranges and needn't reach their ends.
Inputs may be any that keep to these rules, and one draw needn't show every extreme that they name: `damp_qubits`: the 8 entries are distinct qubits.
All inputs are finite; a program needn't handle non-finite values.
Results may differ from the reference program's by a relative error of at most 0.00022.
Values sent between devices are 32-bit elements; how exact they have to be, the bound alone decides.
No kernel may reach another device: no remote copies, remote signals or barrier semaphores. Data moves between devices by JAX's collectives and lax.ppermute only.
A program may use at most 128 MiB of HBM per device.

```python
import math
import jax
import jax.numpy as jnp
from jax import lax

AMP_DEV = 131072
LAYERS = 2
KRAUS = 4
AMPS = 16777216
LQ = 17
QUBITS = 24


def draw_initial_state(key, part):
    first_key, second_key = jax.random.split(jax.random.fold_in(key, 17))
    devices = AMPS // AMP_DEV
    positions = lax.iota(jnp.int32, AMPS)
    device_pos = (positions // AMP_DEV).astype(jnp.float32)
    ramp = 2.0 * device_pos / max(devices - 1, 1) - 1.0
    tilts = jax.random.uniform(second_key, (LQ,), jnp.float32, -0.15, 0.15)
    noise = jnp.clip(jax.random.normal(first_key, (2, AMPS), jnp.float32), -5.0, 5.0)
    exponent = jnp.zeros((AMPS,), jnp.float32)
    for qubit_no in range(LQ):
        bit_value = jnp.bitwise_and(jnp.right_shift(positions, qubit_no), 1).astype(jnp.float32)
        exponent = exponent + (bit_value - 0.5) * tilts[qubit_no]
    magnitude = jnp.exp(ramp * (0.55 + 2.0 * exponent))
    return noise * magnitude[None, :]


def draw_damp_qubits(key, part):
    shuffled = jax.random.permutation(jax.random.fold_in(key, 29), LQ)
    return shuffled[:LAYERS * KRAUS].reshape(LAYERS, KRAUS).astype(jnp.int32)


def touch_ends(drawn, rng, least, high):
    longest = drawn.shape.index(max(drawn.shape))
    spots = []
    for shift in (0, 1):
        where = [jax.random.randint(jax.random.fold_in(rng, axis), (), 0, length) for axis, length in enumerate(drawn.shape)]
        where[longest] = (where[longest] + shift) % drawn.shape[longest]
        spots.append(tuple(where))
    return drawn.at[spots[0]].set(least).at[spots[1]].set(high)


def setup_inputs(seed: int = 0) -> dict:
    key_list = jax.random.split(jax.random.key(seed), 6)
    return {
        "initial_state": draw_initial_state(jax.random.fold_in(key_list[5], 71), 0),
        "gate_angles": jnp.clip(jax.random.uniform(key_list[1], (LAYERS, 3, QUBITS), jnp.float32, -3.140625, 3.140625), -3.140625, 3.140625),
        "damp_qubits": draw_damp_qubits(jax.random.fold_in(key_list[5], 71), 0),
        "kraus_branch": touch_ends((jax.random.randint(key_list[3], (LAYERS, KRAUS), 0, 5) < 2).astype(jnp.int32), jax.random.fold_in(key_list[3], 1), 0, 1),
        "damping": jnp.clip(jnp.exp(jax.random.uniform(key_list[4], (LAYERS, KRAUS), jnp.float32, math.log(0.1), math.log(0.6))), 0.1, 0.6),
    }


epsilon = 1e-06

def gate_table(angles):
    half_theta = angles[1] * 0.5
    cosine = jnp.cos(half_theta)
    sine = jnp.sin(half_theta)
    summed = (angles[0] + angles[2]) * 0.5
    differ = (angles[0] - angles[2]) * 0.5
    real_part = jnp.stack([jnp.stack([jnp.cos(summed) * cosine, -jnp.cos(differ) * sine]), jnp.stack([jnp.cos(differ) * sine, jnp.cos(summed) * cosine])])
    imag_part = jnp.stack([jnp.stack([-jnp.sin(summed) * cosine, jnp.sin(differ) * sine]), jnp.stack([jnp.sin(differ) * sine, jnp.sin(summed) * cosine])])
    return (real_part, imag_part)

def complex_times(coef_re, coef_im, values):
    return jnp.stack([coef_re * values[0] - coef_im * values[1], coef_re * values[1] + coef_im * values[0]])

def apply_gate(amplitudes, position, real_part, imag_part):
    total = amplitudes.shape[1]
    viewed = amplitudes.reshape(2, total >> position + 1, 2, 1 << position)
    zero_half = viewed[:, :, 0]
    one_half = viewed[:, :, 1]
    new_zero = complex_times(real_part[0, 0], imag_part[0, 0], zero_half) + complex_times(real_part[0, 1], imag_part[0, 1], one_half)
    new_one = complex_times(real_part[1, 0], imag_part[1, 0], zero_half) + complex_times(real_part[1, 1], imag_part[1, 1], one_half)
    return jnp.stack([new_zero, new_one], axis=2).reshape(2, total)

def damp_step(amplitudes, target, rate, branch):
    total = amplitudes.shape[1]
    positions = lax.iota(jnp.int32, total)
    low_bit = jnp.bitwise_and(jnp.right_shift(positions, target), 1) == 0
    stride = jnp.left_shift(jnp.int32(1), target)
    shifted = jnp.roll(amplitudes, -stride, axis=1)
    lowered = jnp.where(low_bit, jnp.sqrt(rate) * shifted, jnp.zeros_like(amplitudes))
    kept = jnp.where(low_bit, amplitudes, jnp.sqrt(1.0 - rate) * amplitudes)
    return jnp.where(branch == 1, lowered, kept)

def reference(initial_state, gate_angles, damp_qubits, kraus_branch, damping):
    amplitudes = initial_state
    weights = []
    for layer_no in range(LAYERS):
        real_part, imag_part = gate_table(gate_angles[layer_no])
        for qubit_no in range(QUBITS):
            amplitudes = apply_gate(amplitudes, qubit_no, real_part[:, :, qubit_no], imag_part[:, :, qubit_no])
        for slot_no in range(KRAUS):
            before = jnp.sum(amplitudes * amplitudes) / AMPS
            damped = damp_step(amplitudes, damp_qubits[layer_no, slot_no], damping[layer_no, slot_no], kraus_branch[layer_no, slot_no])
            after = jnp.sum(damped * damped) / AMPS
            weights.append(after / before)
            amplitudes = damped * lax.rsqrt(after + epsilon)
    return (amplitudes, jnp.stack(weights).reshape(LAYERS, KRAUS))
```

```python
import functools

import jax
import jax.numpy as jnp
from jax import lax
from jax.experimental import pallas as pl
from jax.experimental.pallas import tpu as pltpu
from jax.sharding import PartitionSpec as P

AXES = ("hi", "lo")
EPS = 1e-6
LANES = 128
ROWS = 16
MID = 8
f32 = jnp.float32
bf16 = jnp.bfloat16


def split(x):
    hi = x.astype(bf16)
    return hi, (x - hi.astype(f32)).astype(bf16)


def dot3(a, b):
    (ah, al), (bh, bl) = a, b
    d = functools.partial(jnp.dot, preferred_element_type=f32)
    return d(ah, bh) + (d(ah, bl) + d(al, bh))


def cmul(a, b):
    return a[0] * b[0] - a[1] * b[1], a[0] * b[1] + a[1] * b[0]


def matmul2(a, b):
    out = {}
    for i in range(2):
        for j in range(2):
            p, q = cmul(a[i, 0], b[0, j]), cmul(a[i, 1], b[1, j])
            out[i, j] = (p[0] + q[0], p[1] + q[1])
    return out


def scale2(k, u):
    k00, k01, k11 = k
    out = {}
    for j in range(2):
        out[0, j] = tuple(k00 * u[0, j][c] + k01 * u[1, j][c] for c in range(2))
        out[1, j] = tuple(k11 * u[1, j][c] for c in range(2))
    return out


def gates(angles_ref, layer):
    a, b, c = (angles_ref[layer, k : k + 1, :] for k in range(3))
    co, si = jnp.cos(b * 0.5), jnp.sin(b * 0.5)
    s, d = (a + c) * 0.5, (a - c) * 0.5
    cs, ss, cd, sd = jnp.cos(s), jnp.sin(s), jnp.cos(d), jnp.sin(d)
    return {
        (0, 0): (cs * co, -ss * co),
        (0, 1): (-cd * si, sd * si),
        (1, 0): (cd * si, sd * si),
        (1, 1): (cs * co, ss * co),
    }


def tables(angles_ref, targets, branches, rates):
    qubits = angles_ref.shape[2]
    lane = lax.broadcasted_iota(jnp.int32, (1, qubits), 1)
    one, zero = jnp.ones((1, qubits), f32), jnp.zeros((1, qubits), f32)
    u = [gates(angles_ref, layer) for layer in range(2)]
    krauses, first = [], zero > 1.0
    for layer in range(2):
        k00, k01, k11 = one, zero, one
        for slot in range(4):
            here = lane == targets[layer, slot]
            jump = branches[layer, slot] == 1
            g = jnp.full((1, qubits), rates[layer, slot], f32)
            k00 = jnp.where(here, jnp.where(jump, 0.0, 1.0), k00)
            k01 = jnp.where(here, jnp.where(jump, jnp.sqrt(g), 0.0), k01)
            k11 = jnp.where(here, jnp.where(jump, 0.0, jnp.sqrt(1.0 - g)), k11)
            if layer == 0:
                first = jnp.logical_or(first, here)
        krauses.append((k00, k01, k11))
    both = matmul2(u[1], u[0])
    v = {
        ij: tuple(jnp.where(first, u[0][ij][c], both[ij][c]) for c in range(2))
        for ij in both
    }
    m = scale2(krauses[1], matmul2(u[1], scale2(krauses[0], u[0])))
    return v, m


def entry(table, ij, c, qubit):
    return table[ij][c][:, qubit : qubit + 1]


def kron(table, start, transposed):
    rows = lax.broadcasted_iota(jnp.int32, (LANES, LANES), 0)
    cols = lax.broadcasted_iota(jnp.int32, (LANES, LANES), 1)
    if transposed:
        rows, cols = cols, rows
    acc = None
    for j in range(7):
        rb = jnp.bitwise_and(rows, 1 << j) == 0
        cb = jnp.bitwise_and(cols, 1 << j) == 0
        e = []
        for c in range(2):
            w = {
                ij: jnp.broadcast_to(entry(table, ij, c, start + j), (LANES, LANES))
                for ij in table
            }
            e.append(
                jnp.where(
                    rb,
                    jnp.where(cb, w[0, 0], w[0, 1]),
                    jnp.where(cb, w[1, 0], w[1, 1]),
                )
            )
        acc = tuple(e) if acc is None else cmul(acc, e)
    return acc


def left_big(w):
    re, im = w
    return jnp.concatenate(
        [jnp.concatenate([re, -im], 1), jnp.concatenate([im, re], 1)], 0
    )


def right_big(w):
    re, im = w
    return jnp.concatenate(
        [jnp.concatenate([re, im], 1), jnp.concatenate([-im, re], 1)], 0
    )


def mid_mix(load, store, coef):
    x = [load(q) for q in range(MID)]
    for j in range(3):
        for q in range(MID):
            if q >> j & 1:
                continue
            p = q | 1 << j
            x0, x1 = x[q], x[p]
            new = []
            for i in range(2):
                a, b = cmul(coef(j, i, 0), x0), cmul(coef(j, i, 1), x1)
                new.append((a[0] + b[0], a[1] + b[1]))
            x[q], x[p] = new
    for q in range(MID):
        store(q, x[q])


def strided(start, stride):
    return pl.ds(start, LANES, stride=stride)


def right_stage(x_ref, stride, weights, tmp_ref):
    for q in range(MID):
        x = jnp.concatenate(
            [x_ref[strided(2 * q + c, stride), :] for c in range(2)], 1
        )
        tmp_ref[q] = dot3(split(x), weights)


def mid_stage(tmp_ref, coef):
    def body(i, _):
        at = pl.ds(pl.multiple_of(i * 8, 8), 8)

        def load(q):
            return tmp_ref[q, at, :LANES], tmp_ref[q, at, LANES:]

        def store(q, value):
            tmp_ref[q, at, :LANES], tmp_ref[q, at, LANES:] = value

        mid_mix(load, store, coef)
        return 0

    lax.fori_loop(0, LANES // 8, body, 0, unroll=True)


def left_pair(weights, a, b):
    x = jnp.concatenate(
        [jnp.concatenate([a[c], b[c]], 1) for c in range(2)], 0
    )
    y = dot3(weights, split(x))
    return [
        tuple(y[c * LANES : (c + 1) * LANES, p * LANES : (p + 1) * LANES] for c in range(2))
        for p in range(2)
    ]


def level_sums(squares, targets, branches, rates, layer):
    lane = lax.broadcasted_iota(jnp.int32, (LANES, LANES), 1)
    row = lax.broadcasted_iota(jnp.int32, (LANES, LANES), 0)
    weight = jnp.ones((LANES, LANES), f32)
    wq = [jnp.float32(1.0)] * MID
    out = []

    def total(v):
        return jnp.sum(jnp.sum(v, axis=0, keepdims=True), axis=1, keepdims=True)

    for slot in range(5):
        mixed = wq[0] * squares[0]
        for q in range(1, MID):
            mixed = mixed + wq[q] * squares[q]
        out.append(total(mixed * weight))
        if slot == 4:
            break
        t = targets[layer, slot]
        g = rates[layer, slot]
        jump = branches[layer, slot] == 1
        f0 = jnp.where(jump, 0.0, 1.0)
        f1 = jnp.where(jump, g, 1.0 - g)
        low, mid = t < 7, jnp.logical_and(t >= 7, t < 10)
        index = jnp.where(low, lane, row)
        shift = jnp.where(low, t, jnp.maximum(t - 10, 0))
        bit = jnp.bitwise_and(jnp.right_shift(index, shift), 1)
        factor = jnp.where(bit == 1, f1, f0)
        weight = weight * jnp.where(mid, jnp.ones_like(factor), factor)
        tm = jnp.where(mid, t - 7, 0)
        wq = [
            w * jnp.where(mid, jnp.where(jnp.bitwise_and(jnp.right_shift(q, tm), 1) == 1, f1, f0), 1.0)
            for q, w in enumerate(wq)
        ]
    return out, weight, wq


def prep_kernel(x_ref, angles_ref, targets, branches, rates,
                g_ref, low_ref, top_ref, mid_ref, sums_ref, tmp_ref):
    v, m = tables(angles_ref, targets, branches, rates)
    g_ref[0], g_ref[1] = split(left_big(kron(m, 17, False)))
    low_ref[0], low_ref[1] = split(right_big(kron(m, 0, True)))
    top_ref[0], top_ref[1] = split(left_big(kron(m, 10, False)))
    for j in range(3):
        for i in range(2):
            for k in range(2):
                for c in range(2):
                    r = ((j * 2 + i) * 2 + k) * 2 + c
                    mid_ref[r : r + 1, :] = jnp.broadcast_to(
                        entry(m, (i, k), c, 7 + j), (1, LANES)
                    )
    v_low = split(right_big(kron(v, 0, True)))
    v_top = split(left_big(kron(v, 10, False)))
    right_stage(x_ref, ROWS, v_low, tmp_ref)
    v_mid = {
        (j, i, k, c): jnp.broadcast_to(entry(v, (i, k), c, 7 + j), (8, LANES))
        for j in range(3) for i in range(2) for k in range(2) for c in range(2)
    }
    mid_stage(tmp_ref, lambda j, i, k: (v_mid[j, i, k, 0], v_mid[j, i, k, 1]))
    psi = []
    for q in range(0, MID, 2):
        ab = [(tmp_ref[p, :, :LANES], tmp_ref[p, :, LANES:]) for p in (q, q + 1)]
        for p, y in zip((q, q + 1), left_pair(v_top, *ab)):
            tmp_ref[p, :, :LANES], tmp_ref[p, :, LANES:] = y
    squares = [
        tmp_ref[q, :, :LANES] * tmp_ref[q, :, :LANES]
        + tmp_ref[q, :, LANES:] * tmp_ref[q, :, LANES:]
        for q in range(MID)
    ]
    first, weight, wq = level_sums(squares, targets, branches, rates, 0)
    kept = first[4]
    alpha = jnp.where(kept > 0.0, lax.rsqrt(jnp.maximum(kept, 1e-37)), 0.0)
    root = jnp.sqrt(weight)
    later = []
    for q in range(MID):
        r = root * jnp.sqrt(jnp.full((1, LANES), wq[q], f32)) * alpha
        re, im = tmp_ref[q, :, :LANES] * r, tmp_ref[q, :, LANES:] * r
        later.append(re * re + im * im)
    second, _, _ = level_sums(later, targets, branches, rates, 1)
    base = jnp.where(second[0] > 0.0, second[0], 1.0)
    values = first + [s / base for s in second[1:]]
    lane = lax.broadcasted_iota(jnp.int32, (8, LANES), 1)
    packed = jnp.zeros((8, LANES), f32)
    for k, s in enumerate(values):
        packed = jnp.where(lane == k, s, packed)
    sums_ref[...] = packed


def global_kernel(x_ref, g_ref, sums_ref, out_ref, *, stride):
    weights = (g_ref[0], g_ref[1])
    for q in range(0, MID, 2):
        ab = [
            tuple(x_ref[strided(2 * p + c, ROWS), :] for c in range(2))
            for p in (q, q + 1)
        ]
        for p, y in zip((q, q + 1), left_pair(weights, *ab)):
            for c in range(2):
                out_ref[strided(2 * p + c, stride), :] = y[c]
    out_ref[strided(ROWS, stride), :] = jnp.broadcast_to(
        sums_ref[0:1, :], (LANES, LANES)
    )


def final_kernel(x_ref, low_ref, top_ref, mid_ref, out_ref, weights_ref, tmp_ref, *, stride, whole):
    parts = x_ref[strided(ROWS, stride), :]
    totals = jnp.sum(parts, axis=0, keepdims=True)
    kept = parts[:, 4:5]
    kept_total = jnp.maximum(totals[:, 4:5], 1e-37)
    ratios = jnp.sum(parts * (kept / kept_total), axis=0, keepdims=True)
    lane = lax.broadcasted_iota(jnp.int32, (1, LANES), 1)
    row = jnp.zeros((1, LANES), f32)
    factors = []
    mean = [totals[:, k : k + 1] / whole for k in range(5)]
    for layer in range(2):
        factor = jnp.ones((1, 1), f32)
        for slot in range(4):
            before = mean[slot] * factor * factor
            after = mean[slot + 1] * factor * factor
            row = jnp.where(lane == layer * 4 + slot, after / before, row)
            factor = factor * lax.rsqrt(after + EPS)
        factors.append(factor)
        if layer == 0:
            start = mean[4] * factor * factor
            mean = [start] + [start * ratios[:, 5 + k : 6 + k] for k in range(4)]
    weights_ref[...] = jnp.broadcast_to(row, (8, LANES))
    right_stage(x_ref, stride, (low_ref[0], low_ref[1]), tmp_ref)

    def coef(j, i, k):
        r = ((j * 2 + i) * 2 + k) * 2
        return mid_ref[r : r + 1, :], mid_ref[r + 1 : r + 2, :]

    mid_stage(tmp_ref, coef)
    top = (top_ref[0], top_ref[1])
    for q in range(0, MID, 2):
        ab = [(tmp_ref[p, :, :LANES], tmp_ref[p, :, LANES:]) for p in (q, q + 1)]
        for p, y in zip((q, q + 1), left_pair(top, *ab)):
            for c in range(2):
                out_ref[strided(2 * p + c, ROWS), :] = y[c] * factors[0] * factors[1]


def on_device(initial_state, gate_angles, damp_qubits, kraus_branch, damping):
    devices = lax.axis_size(AXES)
    local = initial_state.shape[1]
    whole = float(local * devices)
    stride = ROWS + 1
    vmem = pl.BlockSpec(memory_space=pltpu.VMEM)
    smem = pl.BlockSpec(memory_space=pltpu.SMEM)
    rows = local * 2 // LANES
    x = initial_state.reshape(2, rows // 2, LANES).transpose(1, 0, 2)
    x = x.reshape(devices, ROWS, LANES)
    swapped = lax.all_to_all(x, AXES, split_axis=0, concat_axis=0, tiled=True)
    big = jax.ShapeDtypeStruct((2, 256, 256), bf16)
    g, low, top, mid, sums = pl.pallas_call(
        prep_kernel,
        out_shape=(big, big, big,
                   jax.ShapeDtypeStruct((24, LANES), f32),
                   jax.ShapeDtypeStruct((8, LANES), f32)),
        in_specs=[vmem, vmem, smem, smem, smem],
        out_specs=(vmem,) * 5,
        scratch_shapes=[pltpu.VMEM((MID, LANES, 2 * LANES), f32)],
        cost_estimate=pl.CostEstimate(flops=2_000_000_000, bytes_accessed=2_000_000, transcendentals=0),
        name="prep",
    )(x.reshape(rows, LANES), gate_angles, damp_qubits, kraus_branch, damping)
    mixed = pl.pallas_call(
        functools.partial(global_kernel, stride=stride),
        out_shape=jax.ShapeDtypeStruct((devices * stride, LANES), f32),
        in_specs=[vmem] * 3,
        out_specs=vmem,
        cost_estimate=pl.CostEstimate(flops=400_000_000, bytes_accessed=2_000_000, transcendentals=0),
        name="global_gates",
    )(swapped.reshape(rows, LANES), g, sums)
    back = lax.all_to_all(
        mixed.reshape(devices, 1, stride * LANES), AXES, split_axis=0, concat_axis=0, tiled=True
    )
    out, weights = pl.pallas_call(
        functools.partial(final_kernel, stride=stride, whole=whole),
        out_shape=(jax.ShapeDtypeStruct((rows, LANES), f32),
                   jax.ShapeDtypeStruct((8, LANES), f32)),
        in_specs=[vmem] * 4,
        out_specs=(vmem, vmem),
        scratch_shapes=[pltpu.VMEM((MID, LANES, 2 * LANES), f32)],
        cost_estimate=pl.CostEstimate(flops=800_000_000, bytes_accessed=2_000_000, transcendentals=0),
        name="local_gates",
    )(back.reshape(devices * stride, LANES), low, top, mid)
    out = out.reshape(rows // 2, 2, LANES).transpose(1, 0, 2).reshape(2, local)
    return out, weights[0, : damp_qubits.size].reshape(damp_qubits.shape)


def solution(mesh):
    return jax.shard_map(
        on_device,
        mesh=mesh,
        in_specs=(P(None, AXES), P(), P(), P(), P()),
        out_specs=(P(None, AXES), P()),
        check_vma=False,
    )
```

```python
import functools

import jax
import jax.numpy as jnp
from jax import lax
from jax.experimental import pallas as pl
from jax.experimental.pallas import tpu as pltpu
from jax.sharding import PartitionSpec as P

AXES = ("hi", "lo")
EPS = 1e-6
LANES = 128
ROWS = 16
MID = 8
f32 = jnp.float32
bf16 = jnp.bfloat16


def split(x):
    hi = x.astype(bf16)
    return hi, (x - hi.astype(f32)).astype(bf16)


def dot3(a, b):
    (ah, al), (bh, bl) = a, b
    d = functools.partial(jnp.dot, preferred_element_type=f32)
    return d(ah, bh) + (d(ah, bl) + d(al, bh))


def cmul(a, b):
    return a[0] * b[0] - a[1] * b[1], a[0] * b[1] + a[1] * b[0]


def matmul2(a, b):
    out = {}
    for i in range(2):
        for j in range(2):
            p, q = cmul(a[i, 0], b[0, j]), cmul(a[i, 1], b[1, j])
            out[i, j] = (p[0] + q[0], p[1] + q[1])
    return out


def scale2(k, u):
    k00, k01, k11 = k
    out = {}
    for j in range(2):
        out[0, j] = tuple(k00 * u[0, j][c] + k01 * u[1, j][c] for c in range(2))
        out[1, j] = tuple(k11 * u[1, j][c] for c in range(2))
    return out


def gates(angles_ref, layer):
    a, b, c = (angles_ref[layer, k : k + 1, :] for k in range(3))
    co, si = jnp.cos(b * 0.5), jnp.sin(b * 0.5)
    s, d = (a + c) * 0.5, (a - c) * 0.5
    cs, ss, cd, sd = jnp.cos(s), jnp.sin(s), jnp.cos(d), jnp.sin(d)
    return {
        (0, 0): (cs * co, -ss * co),
        (0, 1): (-cd * si, sd * si),
        (1, 0): (cd * si, sd * si),
        (1, 1): (cs * co, ss * co),
    }


def tables(angles_ref, targets, branches, rates):
    qubits = angles_ref.shape[2]
    lane = lax.broadcasted_iota(jnp.int32, (1, qubits), 1)
    one, zero = jnp.ones((1, qubits), f32), jnp.zeros((1, qubits), f32)
    u = [gates(angles_ref, layer) for layer in range(2)]
    krauses, first = [], zero > 1.0
    for layer in range(2):
        k00, k01, k11 = one, zero, one
        for slot in range(4):
            here = lane == targets[layer, slot]
            jump = branches[layer, slot] == 1
            g = jnp.full((1, qubits), rates[layer, slot], f32)
            k00 = jnp.where(here, jnp.where(jump, 0.0, 1.0), k00)
            k01 = jnp.where(here, jnp.where(jump, jnp.sqrt(g), 0.0), k01)
            k11 = jnp.where(here, jnp.where(jump, 0.0, jnp.sqrt(1.0 - g)), k11)
            if layer == 0:
                first = jnp.logical_or(first, here)
        krauses.append((k00, k01, k11))
    both = matmul2(u[1], u[0])
    v = {
        ij: tuple(jnp.where(first, u[0][ij][c], both[ij][c]) for c in range(2))
        for ij in both
    }
    m = scale2(krauses[1], matmul2(u[1], scale2(krauses[0], u[0])))
    return v, m


def entry(table, ij, c, qubit):
    return table[ij][c][:, qubit : qubit + 1]


def kron(table, start, transposed):
    rows = lax.broadcasted_iota(jnp.int32, (LANES, LANES), 0)
    cols = lax.broadcasted_iota(jnp.int32, (LANES, LANES), 1)
    if transposed:
        rows, cols = cols, rows
    acc = None
    for j in range(7):
        rb = jnp.bitwise_and(rows, 1 << j) == 0
        cb = jnp.bitwise_and(cols, 1 << j) == 0
        e = []
        for c in range(2):
            w = {
                ij: jnp.broadcast_to(entry(table, ij, c, start + j), (LANES, LANES))
                for ij in table
            }
            e.append(
                jnp.where(
                    rb,
                    jnp.where(cb, w[0, 0], w[0, 1]),
                    jnp.where(cb, w[1, 0], w[1, 1]),
                )
            )
        acc = tuple(e) if acc is None else cmul(acc, e)
    return acc


def left_big(w):
    re, im = w
    return jnp.concatenate(
        [jnp.concatenate([re, -im], 1), jnp.concatenate([im, re], 1)], 0
    )


def right_big(w):
    re, im = w
    return jnp.concatenate(
        [jnp.concatenate([re, im], 1), jnp.concatenate([-im, re], 1)], 0
    )


def mid_mix(load, store, coef):
    x = [load(q) for q in range(MID)]
    for j in range(3):
        for q in range(MID):
            if q >> j & 1:
                continue
            p = q | 1 << j
            x0, x1 = x[q], x[p]
            new = []
            for i in range(2):
                a, b = cmul(coef(j, i, 0), x0), cmul(coef(j, i, 1), x1)
                new.append((a[0] + b[0], a[1] + b[1]))
            x[q], x[p] = new
    for q in range(MID):
        store(q, x[q])


def strided(start, stride):
    return pl.ds(start, LANES, stride=stride)


def right_stage(x_ref, stride, weights, tmp_ref):
    for q in range(MID):
        x = jnp.concatenate(
            [x_ref[strided(2 * q + c, stride), :] for c in range(2)], 1
        )
        tmp_ref[q] = dot3(split(x), weights)


def mid_stage(tmp_ref, coef):
    def body(i, _):
        at = pl.ds(pl.multiple_of(i * 8, 8), 8)

        def load(q):
            return tmp_ref[q, at, :LANES], tmp_ref[q, at, LANES:]

        def store(q, value):
            tmp_ref[q, at, :LANES], tmp_ref[q, at, LANES:] = value

        mid_mix(load, store, coef)
        return 0

    lax.fori_loop(0, LANES // 8, body, 0, unroll=True)


def left_pair(weights, a, b):
    x = jnp.concatenate(
        [jnp.concatenate([a[c], b[c]], 1) for c in range(2)], 0
    )
    y = dot3(weights, split(x))
    return [
        tuple(y[c * LANES : (c + 1) * LANES, p * LANES : (p + 1) * LANES] for c in range(2))
        for p in range(2)
    ]


def level_sums(squares, targets, branches, rates, layer):
    lane = lax.broadcasted_iota(jnp.int32, (LANES, LANES), 1)
    row = lax.broadcasted_iota(jnp.int32, (LANES, LANES), 0)
    weight = jnp.ones((LANES, LANES), f32)
    wq = [jnp.float32(1.0)] * MID
    out = []

    def total(v):
        return jnp.sum(jnp.sum(v, axis=0, keepdims=True), axis=1, keepdims=True)

    for slot in range(5):
        mixed = wq[0] * squares[0]
        for q in range(1, MID):
            mixed = mixed + wq[q] * squares[q]
        out.append(total(mixed * weight))
        if slot == 4:
            break
        t = targets[layer, slot]
        g = rates[layer, slot]
        jump = branches[layer, slot] == 1
        f0 = jnp.where(jump, 0.0, 1.0)
        f1 = jnp.where(jump, g, 1.0 - g)
        low, mid = t < 7, jnp.logical_and(t >= 7, t < 10)
        index = jnp.where(low, lane, row)
        shift = jnp.where(low, t, jnp.maximum(t - 10, 0))
        bit = jnp.bitwise_and(jnp.right_shift(index, shift), 1)
        factor = jnp.where(bit == 1, f1, f0)
        weight = weight * jnp.where(mid, jnp.ones_like(factor), factor)
        tm = jnp.where(mid, t - 7, 0)
        wq = [
            w * jnp.where(mid, jnp.where(jnp.bitwise_and(jnp.right_shift(q, tm), 1) == 1, f1, f0), 1.0)
            for q, w in enumerate(wq)
        ]
    return out, weight, wq


def prep_kernel(x_ref, angles_ref, targets, branches, rates,
                g_ref, low_ref, top_ref, mid_ref, sums_ref, tmp_ref):
    v, m = tables(angles_ref, targets, branches, rates)
    g_ref[0], g_ref[1] = split(left_big(kron(m, 17, False)))
    low_ref[0], low_ref[1] = split(right_big(kron(m, 0, True)))
    top_ref[0], top_ref[1] = split(left_big(kron(m, 10, False)))
    for j in range(3):
        for i in range(2):
            for k in range(2):
                for c in range(2):
                    r = ((j * 2 + i) * 2 + k) * 2 + c
                    mid_ref[r : r + 1, :] = jnp.broadcast_to(
                        entry(m, (i, k), c, 7 + j), (1, LANES)
                    )
    v_low = split(right_big(kron(v, 0, True)))
    v_top = split(left_big(kron(v, 10, False)))
    right_stage(x_ref, ROWS, v_low, tmp_ref)
    v_mid = {
        (j, i, k, c): jnp.broadcast_to(entry(v, (i, k), c, 7 + j), (8, LANES))
        for j in range(3) for i in range(2) for k in range(2) for c in range(2)
    }
    mid_stage(tmp_ref, lambda j, i, k: (v_mid[j, i, k, 0], v_mid[j, i, k, 1]))
    psi = []
    for q in range(0, MID, 2):
        ab = [(tmp_ref[p, :, :LANES], tmp_ref[p, :, LANES:]) for p in (q, q + 1)]
        for p, y in zip((q, q + 1), left_pair(v_top, *ab)):
            tmp_ref[p, :, :LANES], tmp_ref[p, :, LANES:] = y
    squares = [
        tmp_ref[q, :, :LANES] * tmp_ref[q, :, :LANES]
        + tmp_ref[q, :, LANES:] * tmp_ref[q, :, LANES:]
        for q in range(MID)
    ]
    first, weight, wq = level_sums(squares, targets, branches, rates, 0)
    kept = first[4]
    alpha = jnp.where(kept > 0.0, lax.rsqrt(jnp.maximum(kept, 1e-37)), 0.0)
    root = jnp.sqrt(weight)
    later = []
    for q in range(MID):
        r = root * jnp.sqrt(jnp.full((1, LANES), wq[q], f32)) * alpha
        re, im = tmp_ref[q, :, :LANES] * r, tmp_ref[q, :, LANES:] * r
        later.append(re * re + im * im)
    second, _, _ = level_sums(later, targets, branches, rates, 1)
    base = jnp.where(second[0] > 0.0, second[0], 1.0)
    values = first + [s / base for s in second[1:]]
    lane = lax.broadcasted_iota(jnp.int32, (8, LANES), 1)
    packed = jnp.zeros((8, LANES), f32)
    for k, s in enumerate(values):
        packed = jnp.where(lane == k, s, packed)
    sums_ref[...] = packed


def global_kernel(x_ref, g_ref, sums_ref, out_ref, *, stride):
    weights = (g_ref[0], g_ref[1])
    for q in range(0, MID, 2):
        ab = [
            tuple(x_ref[strided(2 * p + c, ROWS), :] for c in range(2))
            for p in (q, q + 1)
        ]
        for p, y in zip((q, q + 1), left_pair(weights, *ab)):
            for c in range(2):
                out_ref[strided(2 * p + c, stride), :] = y[c]
    out_ref[strided(ROWS, stride), :] = jnp.broadcast_to(
        sums_ref[0:1, :], (LANES, LANES)
    )


def final_kernel(x_ref, low_ref, top_ref, mid_ref, out_ref, weights_ref, tmp_ref, *, stride, whole):
    parts = x_ref[strided(ROWS, stride), :]
    totals = jnp.sum(parts, axis=0, keepdims=True)
    kept = parts[:, 4:5]
    kept_total = jnp.maximum(totals[:, 4:5], 1e-37)
    ratios = jnp.sum(parts * (kept / kept_total), axis=0, keepdims=True)
    lane = lax.broadcasted_iota(jnp.int32, (1, LANES), 1)
    row = jnp.zeros((1, LANES), f32)
    factors = []
    mean = [totals[:, k : k + 1] / whole for k in range(5)]
    for layer in range(2):
        factor = jnp.ones((1, 1), f32)
        for slot in range(4):
            before = mean[slot] * factor * factor
            after = mean[slot + 1] * factor * factor
            row = jnp.where(lane == layer * 4 + slot, after / before, row)
            factor = factor * lax.rsqrt(after + EPS)
        factors.append(factor)
        if layer == 0:
            start = mean[4] * factor * factor
            mean = [start] + [start * ratios[:, 5 + k : 6 + k] for k in range(4)]
    weights_ref[0:1, :] = row[:, 0:4]
    weights_ref[1:2, :] = row[:, 4:8]
    right_stage(x_ref, stride, (low_ref[0], low_ref[1]), tmp_ref)

    def coef(j, i, k):
        r = ((j * 2 + i) * 2 + k) * 2
        return mid_ref[r : r + 1, :], mid_ref[r + 1 : r + 2, :]

    mid_stage(tmp_ref, coef)
    top = (top_ref[0], top_ref[1])
    for q in range(0, MID, 2):
        ab = [(tmp_ref[p, :, :LANES], tmp_ref[p, :, LANES:]) for p in (q, q + 1)]
        for p, y in zip((q, q + 1), left_pair(top, *ab)):
            for c in range(2):
                out_ref[strided(2 * p + c, ROWS), :] = y[c] * factors[0] * factors[1]


def on_device(initial_state, gate_angles, damp_qubits, kraus_branch, damping):
    devices = lax.axis_size(AXES)
    local = initial_state.shape[1]
    whole = float(local * devices)
    stride = ROWS + 1
    vmem = pl.BlockSpec(memory_space=pltpu.VMEM)
    smem = pl.BlockSpec(memory_space=pltpu.SMEM)
    rows = local * 2 // LANES
    x = initial_state.reshape(2, rows // 2, LANES).transpose(1, 0, 2)
    x = x.reshape(devices, ROWS, LANES)
    swapped = lax.all_to_all(x, AXES, split_axis=0, concat_axis=0, tiled=True)
    big = pltpu.VMEM((2, 256, 256), bf16)
    near = functools.partial(pltpu.with_memory_space_constraint, memory_space=pltpu.VMEM)
    params = pltpu.CompilerParams(vmem_limit_bytes=24 << 20)
    g, low, top, mid, sums = pl.pallas_call(
        prep_kernel,
        out_shape=(big, big, big,
                   pltpu.VMEM((24, LANES), f32),
                   pltpu.VMEM((8, LANES), f32)),
        in_specs=[vmem, vmem, smem, smem, smem],
        out_specs=(vmem,) * 5,
        scratch_shapes=[pltpu.VMEM((MID, LANES, 2 * LANES), f32)],
        cost_estimate=pl.CostEstimate(flops=2_000_000_000, bytes_accessed=2_000_000, transcendentals=0),
        compiler_params=params,
        name="prep",
    )(x.reshape(rows, LANES), gate_angles, damp_qubits, kraus_branch, damping)
    mixed = pl.pallas_call(
        functools.partial(global_kernel, stride=stride),
        out_shape=pltpu.VMEM((devices * stride, LANES), f32),
        in_specs=[vmem] * 3,
        out_specs=vmem,
        cost_estimate=pl.CostEstimate(flops=400_000_000, bytes_accessed=2_000_000, transcendentals=0),
        compiler_params=params,
        name="global_gates",
    )(near(swapped.reshape(rows, LANES)), near(g), near(sums))
    back = lax.all_to_all(
        mixed.reshape(devices, 1, stride * LANES), AXES, split_axis=0, concat_axis=0, tiled=True
    )
    out, weights = pl.pallas_call(
        functools.partial(final_kernel, stride=stride, whole=whole),
        out_shape=(jax.ShapeDtypeStruct((rows, LANES), f32),
                   jax.ShapeDtypeStruct(damp_qubits.shape, f32)),
        in_specs=[vmem] * 4,
        out_specs=(vmem, vmem),
        scratch_shapes=[pltpu.VMEM((MID, LANES, 2 * LANES), f32)],
        cost_estimate=pl.CostEstimate(flops=800_000_000, bytes_accessed=2_000_000, transcendentals=0),
        compiler_params=params,
        name="local_gates",
    )(near(back.reshape(devices * stride, LANES)), near(low), near(top), near(mid))
    out = out.reshape(rows // 2, 2, LANES).transpose(1, 0, 2).reshape(2, local)
    return out, weights


def solution(mesh):
    return jax.shard_map(
        on_device,
        mesh=mesh,
        in_specs=(P(None, AXES), P(), P(), P(), P()),
        out_specs=(P(None, AXES), P()),
        check_vma=False,
    )
```

```python
import functools

import jax
import jax.numpy as jnp
from jax import lax
from jax.experimental import pallas as pl
from jax.experimental.pallas import tpu as pltpu
from jax.sharding import PartitionSpec as P

AXES = ("hi", "lo")
EPS = 1e-6
LANES = 128
ROWS = 16
MID = 8
f32 = jnp.float32
bf16 = jnp.bfloat16


def split(x):
    hi = x.astype(bf16)
    return hi, (x - hi.astype(f32)).astype(bf16)


def dot3(a, b):
    (ah, al), (bh, bl) = a, b
    d = functools.partial(jnp.dot, preferred_element_type=f32)
    return d(ah, bh) + (d(ah, bl) + d(al, bh))


def cmul(a, b):
    return a[0] * b[0] - a[1] * b[1], a[0] * b[1] + a[1] * b[0]


def matmul2(a, b):
    out = {}
    for i in range(2):
        for j in range(2):
            p, q = cmul(a[i, 0], b[0, j]), cmul(a[i, 1], b[1, j])
            out[i, j] = (p[0] + q[0], p[1] + q[1])
    return out


def scale2(k, u):
    k00, k01, k11 = k
    out = {}
    for j in range(2):
        out[0, j] = tuple(k00 * u[0, j][c] + k01 * u[1, j][c] for c in range(2))
        out[1, j] = tuple(k11 * u[1, j][c] for c in range(2))
    return out


def gates(angles_ref):
    a, b, c = (angles_ref[k] for k in range(3))
    half = jnp.concatenate([b, a + c, a - c], 0) * 0.5
    cosine, sine = jnp.cos(half), jnp.sin(half)
    out = []
    for layer in range(2):
        co, cs, cd = (cosine[2 * k + layer : 2 * k + layer + 1] for k in range(3))
        si, ss, sd = (sine[2 * k + layer : 2 * k + layer + 1] for k in range(3))
        out.append({
            (0, 0): (cs * co, -ss * co),
            (0, 1): (-cd * si, sd * si),
            (1, 0): (cd * si, sd * si),
            (1, 1): (cs * co, ss * co),
        })
    return out


def tables(angles_ref, targets, branches, rates):
    qubits = angles_ref.shape[2]
    lane = lax.broadcasted_iota(jnp.int32, (1, qubits), 1)
    one, zero = jnp.ones((1, qubits), f32), jnp.zeros((1, qubits), f32)
    u = gates(angles_ref)
    krauses, first = [], zero > 1.0
    for layer in range(2):
        k00, k01, k11 = one, zero, one
        for slot in range(4):
            here = lane == targets[layer, slot]
            jump = branches[layer, slot] == 1
            g = jnp.full((1, qubits), rates[layer, slot], f32)
            k00 = jnp.where(here, jnp.where(jump, 0.0, 1.0), k00)
            k01 = jnp.where(here, jnp.where(jump, jnp.sqrt(g), 0.0), k01)
            k11 = jnp.where(here, jnp.where(jump, 0.0, jnp.sqrt(1.0 - g)), k11)
            if layer == 0:
                first = jnp.logical_or(first, here)
        krauses.append((k00, k01, k11))
    both = matmul2(u[1], u[0])
    v = {
        ij: tuple(jnp.where(first, u[0][ij][c], both[ij][c]) for c in range(2))
        for ij in both
    }
    w = scale2(krauses[0], u[0])
    m = scale2(krauses[1], matmul2(u[1], w))
    into = [tuple(jnp.where(first, w[0, j][c], m[0, j][c]) for c in range(2)) for j in range(2)]
    rest = ((one, zero), (zero, zero))
    out = [tuple(jnp.where(first, u[1][i, 0][c], rest[i][c]) for c in range(2)) for i in range(2)]
    return v, m, into, out


def jumped(targets, branches, levels):
    chosen, count = [jnp.int32(-1)] * levels, jnp.int32(0)
    for layer in range(2):
        for slot in range(4):
            jump = branches[layer, slot] == 1
            for n in range(levels):
                chosen[n] = jnp.where(jnp.logical_and(jump, count == n), targets[layer, slot], chosen[n])
            count = count + jnp.where(jump, 1, 0)
    places = [9 - n for n in range(levels)]
    taken, free = {}, jnp.int32(0)
    for p in places:
        hit = [t == p for t in chosen]
        taken[p] = functools.reduce(jnp.logical_or, hit)
    result, free = [], jnp.int32(0)
    for p in places:
        other, rank = jnp.int32(-1), jnp.int32(0)
        for t in chosen:
            outside = jnp.logical_or(t < 10 - levels, t > 9)
            other = jnp.where(jnp.logical_and(outside, rank == free), t, other)
            rank = rank + jnp.where(outside, 1, 0)
        result.append((p, jnp.where(taken[p], p, other)))
        free = free + jnp.where(taken[p], 0, 1)
    return result


def at_qubit(rows, t):
    lane = lax.broadcasted_iota(jnp.int32, rows[0][0].shape, 1)
    return [
        tuple(
            jnp.broadcast_to(jnp.sum(jnp.where(lane == t, r[c], 0.0), axis=1, keepdims=True), (1, LANES))
            for c in range(2)
        )
        for r in rows
    ]


def moved(m, places):
    lane = lax.broadcasted_iota(jnp.int32, m[0, 0][0].shape, 1)
    out = dict(m)
    for p, t in places:
        here = jnp.logical_and(lane == t, t != p)
        for ij in out:
            out[ij] = tuple(jnp.where(here, m[ij][c][:, p : p + 1], out[ij][c]) for c in range(2))
    return out


def middle_index(m, t, beta):
    bit = jnp.left_shift(jnp.int32(1), t - 7)
    clear = jnp.bitwise_and(m, jnp.bitwise_not(bit))
    return clear + (bit if beta else 0)


def part(c):
    return slice(c * LANES, (c + 1) * LANES)


def two(a, b, x, y):
    p, q = cmul(a, x), cmul(b, y)
    return p[0] + q[0], p[1] + q[1]


def tile_rows(ref, block, tile, c, blocks):
    return pl.ds(tile * 16 * blocks + 2 * block + c, 8, stride=2 * blocks)


class Flat:
    def __init__(self, ref, blocks):
        self.ref, self.blocks = ref, blocks

    def get(self, block, tile, c):
        return self.ref[tile_rows(self.ref, block, tile, c, self.blocks), :]

    def put(self, block, tile, c, value):
        self.ref[tile_rows(self.ref, block, tile, c, self.blocks), :] = value


class Blocks:
    def __init__(self, ref):
        self.ref = ref

    def get(self, block, tile, c):
        return self.ref[block, pl.ds(pl.multiple_of(tile * 8, 8), 8), part(c)]

    def put(self, block, tile, c, value):
        self.ref[block, pl.ds(pl.multiple_of(tile * 8, 8), 8), part(c)] = value


def cases(t, body):
    @pl.when(t < 7)
    def _():
        body("lane", jnp.maximum(t, 0))

    @pl.when(jnp.logical_and(t >= 10, t < 13))
    def _():
        body("row", t - 10)

    @pl.when(t >= 13)
    def _():
        body("tile", t - 13)

    @pl.when(jnp.logical_and(t >= 7, t < 10))
    def _():
        body("middle", t - 7)


def over_tiles(body):
    def step(i, _):
        body(i)
        return 0

    lax.fori_loop(0, LANES // 8, step, 0, unroll=2)


def low_mask(axis, bit):
    index = lax.broadcasted_iota(jnp.int32, (8, LANES), axis)
    return jnp.bitwise_and(index, jnp.left_shift(jnp.int32(1), bit)) == 0


def contract(src, dst, p, t, row):
    half = 1 << (p - 7)

    def run(kind, bit):
        size = jnp.left_shift(jnp.int32(1), bit)
        axis = 1 if kind == "lane" else 0
        low = low_mask(axis, bit)
        length = LANES if kind == "lane" else 8

        def body(i):
            if kind == "tile":
                up = jnp.bitwise_and(i, size) != 0
                zero, one = jnp.bitwise_and(i, jnp.bitwise_not(size)), jnp.bitwise_or(i, size)
            for m in range(half):
                if kind == "middle":
                    shared = jnp.bitwise_and(jnp.right_shift(m, bit), 1) * half
                    k = [
                        jnp.where(t == p, m + beta * half, middle_index(m, t, beta) + shared)
                        for beta in range(2)
                    ]
                    u, w = ([src.get(n, i, c) for c in range(2)] for n in k)
                elif kind == "tile":
                    k = jnp.where(up, m + half, m)
                    u, w = ([src.get(k, at, c) for c in range(2)] for at in (zero, one))
                else:
                    u, w = [], []
                    for c in range(2):
                        a, b = src.get(m, i, c), src.get(m + half, i, c)
                        u.append(jnp.where(low, a, pltpu.roll(b, size, axis)))
                        w.append(jnp.where(low, pltpu.roll(a, length - size, axis), b))
                for c, value in enumerate(two(row[0], row[1], u, w)):
                    dst.put(m, i, c, value)

        over_tiles(body)

    cases(t, run)


def expand(src, dst, p, t, column):
    half = 1 << (p - 7)

    def run(kind, bit):
        size = jnp.left_shift(jnp.int32(1), bit)
        axis = 1 if kind == "lane" else 0
        low = low_mask(axis, bit)
        length = LANES if kind == "lane" else 8
        if kind in ("lane", "row"):
            e = tuple(jnp.where(low, column[0][c], column[1][c]) for c in range(2))

        def body(i):
            if kind == "tile":
                up = jnp.bitwise_and(i, size) != 0
                at = (jnp.bitwise_and(i, jnp.bitwise_not(size)), jnp.bitwise_or(i, size))
                ei = tuple(jnp.where(up, column[1][c], column[0][c]) for c in range(2))
            for m in range(half):
                if kind == "middle":
                    shared = jnp.bitwise_and(jnp.right_shift(m, bit), 1) * half
                    y = [src.get(m, i, c) for c in range(2)]
                    made = [
                        (jnp.where(t == p, m + beta * half, middle_index(m, t, beta) + shared), cmul(column[beta], y))
                        for beta in range(2)
                    ]
                elif kind == "tile":
                    made = [
                        (m + s * half, cmul(ei, [src.get(m, at[s], c) for c in range(2)]))
                        for s in range(2)
                    ]
                else:
                    y = [src.get(m, i, c) for c in range(2)]
                    s0 = [jnp.where(low, v, pltpu.roll(v, size, axis)) for v in y]
                    s1 = [jnp.where(low, pltpu.roll(v, length - size, axis), v) for v in y]
                    made = [(m, cmul(e, s0)), (m + half, cmul(e, s1))]
                for k, value in made:
                    for c in range(2):
                        dst.put(k, i, c, value[c])

        over_tiles(body)

    cases(t, run)


def entry(table, ij, c, qubit):
    return table[ij][c][:, qubit : qubit + 1]


def store_kron(ref, rows_ref, table, start, right):
    names = ((0, 0), (0, 1), (1, 0), (1, 1))
    for j in range(7):
        for n, ij in enumerate(names):
            for c in range(2):
                r = 8 * j + 2 * n + c
                rows_ref[r : r + 1, :] = jnp.broadcast_to(entry(table, ij, c, start + j), (1, LANES))
    step = 16

    def body(i, _):
        at = pl.multiple_of(i * step, step)
        rows = lax.broadcasted_iota(jnp.int32, (step, LANES), 0) + at
        cols = lax.broadcasted_iota(jnp.int32, (step, LANES), 1)
        if right:
            rows, cols = cols, rows
        acc = None
        for j in range(7):
            rb = jnp.bitwise_and(rows, 1 << j) == 0
            cb = jnp.bitwise_and(cols, 1 << j) == 0
            e = []
            for c in range(2):
                w = [rows_ref[8 * j + 2 * n + c : 8 * j + 2 * n + c + 1, :] for n in range(4)]
                e.append(jnp.where(rb, jnp.where(cb, w[0], w[1]), jnp.where(cb, w[2], w[3])))
            acc = tuple(e) if acc is None else cmul(acc, e)
        for n, (re, im) in enumerate(zip(split(acc[0]), split(acc[1]))):
            here, below = pl.ds(at, step), pl.ds(at + LANES, step)
            ref[n, here, :LANES] = re
            ref[n, below, LANES:] = re
            ref[n, here, LANES:] = im if right else -im
            ref[n, below, :LANES] = -im if right else im
        return 0

    lax.fori_loop(0, LANES // step, body, 0)


def mid_mix(load, store, coef, bits):
    x = [load(q) for q in range(1 << bits)]
    for j in range(bits):
        for q in range(1 << bits):
            if q >> j & 1:
                continue
            p = q | 1 << j
            x0, x1 = x[q], x[p]
            new = []
            for i in range(2):
                a, b = cmul(coef(j, i, 0), x0), cmul(coef(j, i, 1), x1)
                new.append((a[0] + b[0], a[1] + b[1]))
            x[q], x[p] = new
    for q in range(1 << bits):
        store(q, x[q])


def strided(start, stride):
    return pl.ds(start, LANES, stride=stride)


def right_stage(x_ref, stride, weights, tmp_ref, blocks=MID):
    for q in range(blocks):
        x = jnp.concatenate(
            [x_ref[strided(2 * q + c, stride), :] for c in range(2)], 1
        )
        tmp_ref[q] = dot3(split(x), weights)


def left_stage(load, weights, store, blocks=MID):
    for q in range(0, blocks, 2):
        group = range(q, min(q + 2, blocks))
        ys = left_group(weights, [tuple(load(p, c) for c in range(2)) for p in group])
        for p, y in zip(group, ys):
            for c in range(2):
                store(p, c, y[c])


def mid_stage(tmp_ref, coef, bits=3):
    def body(i, _):
        at = pl.ds(pl.multiple_of(i * 8, 8), 8)

        def load(q):
            return tmp_ref[q, at, :LANES], tmp_ref[q, at, LANES:]

        def store(q, value):
            tmp_ref[q, at, :LANES], tmp_ref[q, at, LANES:] = value

        mid_mix(load, store, coef, bits)
        return 0

    lax.fori_loop(0, LANES // 8, body, 0, unroll=2)


def left_group(weights, pairs):
    x = jnp.concatenate([jnp.concatenate([a[c] for a in pairs], 1) for c in range(2)], 0)
    y = dot3(weights, split(x))
    return [
        tuple(y[c * LANES : (c + 1) * LANES, p * LANES : (p + 1) * LANES] for c in range(2))
        for p in range(len(pairs))
    ]


def level_sums(squares, targets, branches, rates, layer):
    lane = lax.broadcasted_iota(jnp.int32, (LANES, LANES), 1)
    row = lax.broadcasted_iota(jnp.int32, (LANES, LANES), 0)
    weight = jnp.ones((LANES, LANES), f32)
    wq = [jnp.float32(1.0)] * MID
    out = []

    def total(v):
        return jnp.sum(jnp.sum(v, axis=0, keepdims=True), axis=1, keepdims=True)

    for slot in range(5):
        mixed = wq[0] * squares[0]
        for q in range(1, MID):
            mixed = mixed + wq[q] * squares[q]
        out.append(total(mixed * weight))
        if slot == 4:
            break
        t = targets[layer, slot]
        g = rates[layer, slot]
        jump = branches[layer, slot] == 1
        f0 = jnp.where(jump, 0.0, 1.0)
        f1 = jnp.where(jump, g, 1.0 - g)
        low, mid = t < 7, jnp.logical_and(t >= 7, t < 10)
        index = jnp.where(low, lane, row)
        shift = jnp.where(low, t, jnp.maximum(t - 10, 0))
        bit = jnp.bitwise_and(jnp.right_shift(index, shift), 1)
        factor = jnp.where(bit == 1, f1, f0)
        weight = weight * jnp.where(mid, jnp.ones_like(factor), factor)
        tm = jnp.where(mid, t - 7, 0)
        wq = [
            w * jnp.where(mid, jnp.where(jnp.bitwise_and(jnp.right_shift(q, tm), 1) == 1, f1, f0), 1.0)
            for q, w in enumerate(wq)
        ]
    return out, weight, wq


def prep_kernel(x_ref, angles_ref, targets, branches, rates,
                g_ref, low_ref, top_ref, mid_ref, sums_ref,
                tmp_ref, rows_ref, low_v_ref, top_v_ref, *, levels):
    v, m, _, out = tables(angles_ref, targets, branches, rates)
    store_kron(g_ref, rows_ref, m, 17, False)
    places = jumped(targets, branches, levels)
    for n, (_, t) in enumerate(places):
        e = at_qubit(out, t)
        for i in range(2):
            for c in range(2):
                r = 24 + 4 * n + 2 * i + c
                mid_ref[r : r + 1, :] = e[i][c]
    m = moved(m, places)
    store_kron(low_ref, rows_ref, m, 0, True)
    store_kron(top_ref, rows_ref, m, 10, False)
    for j in range(3):
        for i in range(2):
            for k in range(2):
                for c in range(2):
                    r = ((j * 2 + i) * 2 + k) * 2 + c
                    mid_ref[r : r + 1, :] = jnp.broadcast_to(
                        entry(m, (i, k), c, 7 + j), (1, LANES)
                    )
    store_kron(low_v_ref, rows_ref, v, 0, True)
    store_kron(top_v_ref, rows_ref, v, 10, False)
    v_low, v_top = ((r[0], r[1]) for r in (low_v_ref, top_v_ref))
    right_stage(x_ref, ROWS, v_low, tmp_ref)
    v_mid = {
        (j, i, k, c): jnp.broadcast_to(entry(v, (i, k), c, 7 + j), (8, LANES))
        for j in range(3) for i in range(2) for k in range(2) for c in range(2)
    }
    mid_stage(tmp_ref, lambda j, i, k: (v_mid[j, i, k, 0], v_mid[j, i, k, 1]))

    def keep(p, c, value):
        tmp_ref[p, :, part(c)] = value

    left_stage(lambda p, c: tmp_ref[p, :, part(c)], v_top, keep)
    squares = [
        tmp_ref[q, :, :LANES] * tmp_ref[q, :, :LANES]
        + tmp_ref[q, :, LANES:] * tmp_ref[q, :, LANES:]
        for q in range(MID)
    ]
    first, weight, wq = level_sums(squares, targets, branches, rates, 0)
    kept = first[4]
    alpha = jnp.where(kept > 0.0, lax.rsqrt(jnp.maximum(kept, 1e-37)), 0.0)
    root = jnp.sqrt(weight)
    later = []
    for q in range(MID):
        r = root * jnp.sqrt(jnp.full((1, LANES), wq[q], f32)) * alpha
        re, im = tmp_ref[q, :, :LANES] * r, tmp_ref[q, :, LANES:] * r
        later.append(re * re + im * im)
    second, _, _ = level_sums(later, targets, branches, rates, 1)
    base = jnp.where(second[0] > 0.0, second[0], 1.0)
    values = first + [s / base for s in second[1:]]
    lane = lax.broadcasted_iota(jnp.int32, (8, LANES), 1)
    packed = jnp.zeros((8, LANES), f32)
    for k, s in enumerate(values):
        packed = jnp.where(lane == k, s, packed)
    sums_ref[...] = packed


def contract_kernel(x_ref, angles_ref, targets, branches, rates, out_ref, *spare, levels):
    _, _, into, _ = tables(angles_ref, targets, branches, rates)
    src = Flat(x_ref, MID)
    for n, (p, t) in enumerate(jumped(targets, branches, levels)):
        dst = Flat(out_ref, MID >> levels) if n == levels - 1 else Blocks(spare[n])
        contract(src, dst, p, t, at_qubit(into, t))
        src = dst


def global_kernel(x_ref, g_ref, sums_ref, out_ref, *, blocks):
    stride = 2 * blocks + 1

    def store(p, c, value):
        out_ref[strided(2 * p + c, stride), :] = value

    left_stage(
        lambda p, c: x_ref[strided(2 * p + c, 2 * blocks), :], (g_ref[0], g_ref[1]), store, blocks
    )
    out_ref[strided(2 * blocks, stride), :] = jnp.broadcast_to(
        sums_ref[0:1, :], (LANES, LANES)
    )


def final_kernel(x_ref, low_ref, top_ref, mid_ref, targets, branches,
                 out_ref, weights_ref, tmp_ref, other_ref, *, levels, whole):
    blocks = MID >> levels
    stride = 2 * blocks + 1
    parts = x_ref[strided(2 * blocks, stride), :]
    totals = jnp.sum(parts, axis=0, keepdims=True)
    kept = parts[:, 4:5]
    kept_total = jnp.maximum(totals[:, 4:5], 1e-37)
    ratios = jnp.sum(parts * (kept / kept_total), axis=0, keepdims=True)
    lane = lax.broadcasted_iota(jnp.int32, (1, LANES), 1)
    row = jnp.zeros((1, LANES), f32)
    factors = []
    mean = [totals[:, k : k + 1] / whole for k in range(5)]
    for layer in range(2):
        factor = jnp.ones((1, 1), f32)
        for slot in range(4):
            before = mean[slot] * factor * factor
            after = mean[slot + 1] * factor * factor
            row = jnp.where(lane == layer * 4 + slot, after / before, row)
            factor = factor * lax.rsqrt(after + EPS)
        factors.append(factor)
        if layer == 0:
            start = mean[4] * factor * factor
            mean = [start] + [start * ratios[:, 5 + k : 6 + k] for k in range(4)]
    weights_ref[0:1, :] = row[:, 0:4]
    weights_ref[1:2, :] = row[:, 4:8]
    right_stage(x_ref, stride, (low_ref[0], low_ref[1]), tmp_ref, blocks)

    def coef(j, i, k):
        r = ((j * 2 + i) * 2 + k) * 2
        return mid_ref[r : r + 1, :], mid_ref[r + 1 : r + 2, :]

    if levels < 3:
        mid_stage(tmp_ref, coef, 3 - levels)

    def store(q, c, value):
        value = value * factors[0] * factors[1]
        if levels:
            tmp_ref[q, :, part(c)] = value
        else:
            out_ref[strided(2 * q + c, ROWS), :] = value

    left_stage(lambda q, c: tmp_ref[q, :, part(c)], (top_ref[0], top_ref[1]), store, blocks)
    src, spare = Blocks(tmp_ref), [other_ref, tmp_ref]
    for n, (p, t) in reversed(list(enumerate(jumped(targets, branches, levels)))):
        r = 24 + 4 * n
        column = [
            tuple(mid_ref[r + 2 * i + c : r + 2 * i + c + 1, :] for c in range(2)) for i in range(2)
        ]
        dst = Flat(out_ref, MID) if n == 0 else Blocks(spare[(levels - 1 - n) % 2])
        expand(src, dst, p, t, column)
        src = dst


def cost(flops):
    return pl.CostEstimate(flops=flops, bytes_accessed=2_000_000, transcendentals=0)


def program(levels, initial_state, gate_angles, damp_qubits, kraus_branch, damping):
    devices = lax.axis_size(AXES)
    local = initial_state.shape[1]
    whole = float(local * devices)
    rows = local * 2 // LANES
    blocks = MID >> levels
    vmem = pl.BlockSpec(memory_space=pltpu.VMEM)
    smem = pl.BlockSpec(memory_space=pltpu.SMEM)
    big = pltpu.VMEM((2, 256, 256), bf16)
    tmp = pltpu.VMEM((MID, LANES, 2 * LANES), f32)
    near = functools.partial(pltpu.with_memory_space_constraint, memory_space=pltpu.VMEM)
    params = pltpu.CompilerParams(vmem_limit_bytes=24 << 20)
    x = initial_state.reshape(2, rows // 2, LANES).transpose(1, 0, 2).reshape(rows, LANES)
    settings = (gate_angles.transpose(1, 0, 2), damp_qubits, kraus_branch, damping)
    table = pltpu.VMEM((2, 256, 256), bf16)
    in_specs = [vmem, vmem, smem, smem, smem]
    sent = x
    if levels:
        sent = pl.pallas_call(
            functools.partial(contract_kernel, levels=levels),
            out_shape=pltpu.VMEM((rows >> levels, LANES), f32),
            in_specs=in_specs,
            out_specs=vmem,
            scratch_shapes=[tmp] * (levels - 1),
            compiler_params=params,
            cost_estimate=cost(20_000_000),
            name=f"contract_{levels}",
        )(near(x), *settings)
    sent = sent.reshape((devices, 1, 2 * blocks * LANES) if levels > 1 else (devices, 2 * blocks, LANES))
    swapped = lax.all_to_all(sent, AXES, split_axis=0, concat_axis=0, tiled=True)
    g, low, top, mid, sums = pl.pallas_call(
        functools.partial(prep_kernel, levels=levels),
        out_shape=(big, big, big, pltpu.VMEM((40, LANES), f32), pltpu.VMEM((8, LANES), f32)),
        in_specs=in_specs,
        out_specs=(vmem,) * 5,
        scratch_shapes=[tmp, pltpu.VMEM((56, LANES), f32), table, table],
        compiler_params=params,
        cost_estimate=cost(2_000_000_000),
        name=f"prep_{levels}",
    )(near(x) if levels else x, *settings)
    mixed = pl.pallas_call(
        functools.partial(global_kernel, blocks=blocks),
        out_shape=pltpu.VMEM((devices * (2 * blocks + 1), LANES), f32),
        in_specs=[vmem] * 3,
        out_specs=vmem,
        compiler_params=params,
        cost_estimate=cost(400_000_000 >> levels),
        name=f"global_gates_{levels}",
    )(near(swapped.reshape(rows >> levels, LANES)), near(g), near(sums))
    back = lax.all_to_all(
        mixed.reshape(devices, 1, (2 * blocks + 1) * LANES), AXES, split_axis=0, concat_axis=0, tiled=True
    )
    out, weights = pl.pallas_call(
        functools.partial(final_kernel, levels=levels, whole=whole),
        out_shape=(jax.ShapeDtypeStruct((rows, LANES), f32),
                   jax.ShapeDtypeStruct(damp_qubits.shape, f32)),
        in_specs=[vmem] * 4 + [smem] * 2,
        out_specs=(vmem, vmem),
        scratch_shapes=[tmp, tmp],
        compiler_params=params,
        cost_estimate=cost(800_000_000),
        name=f"local_gates_{levels}",
    )(near(back.reshape(devices * (2 * blocks + 1), LANES)), near(low), near(top), near(mid),
      damp_qubits, kraus_branch)
    out = out.reshape(rows // 2, 2, LANES).transpose(1, 0, 2).reshape(2, local)
    return out, weights


def on_device(*args):
    kraus_branch = args[3]
    levels = jnp.minimum(jnp.sum(kraus_branch), 3)
    return lax.switch(levels, [functools.partial(program, n) for n in range(4)], *args)


def solution(mesh):
    return jax.shard_map(
        on_device,
        mesh=mesh,
        in_specs=(P(None, AXES), P(), P(), P(), P()),
        out_specs=(P(None, AXES), P()),
        check_vma=False,
    )
```

```python
import functools

import jax
import jax.numpy as jnp
from jax import lax
from jax.experimental import pallas as pl
from jax.experimental.pallas import tpu as pltpu
from jax.sharding import PartitionSpec as P

AXES = ("hi", "lo")
EPS = 1e-6
LANES = 128
ROWS = 16
MID = 8
f32 = jnp.float32
bf16 = jnp.bfloat16


def split(x):
    hi = x.astype(bf16)
    return hi, (x - hi.astype(f32)).astype(bf16)


def dot3(a, b):
    (ah, al), (bh, bl) = a, b
    return jnp.dot(
        jnp.concatenate([ah, ah, al], 1),
        jnp.concatenate([bh, bl, bh], 0),
        preferred_element_type=f32,
    )


def cmul(a, b):
    return a[0] * b[0] - a[1] * b[1], a[0] * b[1] + a[1] * b[0]


def matmul2(a, b):
    out = {}
    for i in range(2):
        for j in range(2):
            p, q = cmul(a[i, 0], b[0, j]), cmul(a[i, 1], b[1, j])
            out[i, j] = (p[0] + q[0], p[1] + q[1])
    return out


def scale2(k, u):
    k00, k01, k11 = k
    out = {}
    for j in range(2):
        out[0, j] = tuple(k00 * u[0, j][c] + k01 * u[1, j][c] for c in range(2))
        out[1, j] = tuple(k11 * u[1, j][c] for c in range(2))
    return out


def gates(angles_ref):
    a, b, c = (angles_ref[k] for k in range(3))
    half = jnp.concatenate([b, a + c, a - c], 0) * 0.5
    cosine, sine = jnp.cos(half), jnp.sin(half)
    out = []
    for layer in range(2):
        co, cs, cd = (cosine[2 * k + layer : 2 * k + layer + 1] for k in range(3))
        si, ss, sd = (sine[2 * k + layer : 2 * k + layer + 1] for k in range(3))
        out.append({
            (0, 0): (cs * co, -ss * co),
            (0, 1): (-cd * si, sd * si),
            (1, 0): (cd * si, sd * si),
            (1, 1): (cs * co, ss * co),
        })
    return out


def tables(angles_ref, targets, branches, rates):
    qubits = angles_ref.shape[2]
    lane = lax.broadcasted_iota(jnp.int32, (1, qubits), 1)
    one, zero = jnp.ones((1, qubits), f32), jnp.zeros((1, qubits), f32)
    u = gates(angles_ref)
    krauses, first = [], zero > 1.0
    for layer in range(2):
        k00, k01, k11 = one, zero, one
        for slot in range(4):
            here = lane == targets[layer, slot]
            jump = branches[layer, slot] == 1
            g = jnp.full((1, qubits), rates[layer, slot], f32)
            k00 = jnp.where(here, jnp.where(jump, 0.0, 1.0), k00)
            k01 = jnp.where(here, jnp.where(jump, jnp.sqrt(g), 0.0), k01)
            k11 = jnp.where(here, jnp.where(jump, 0.0, jnp.sqrt(1.0 - g)), k11)
            if layer == 0:
                first = jnp.logical_or(first, here)
        krauses.append((k00, k01, k11))
    both = matmul2(u[1], u[0])
    v = {
        ij: tuple(jnp.where(first, u[0][ij][c], both[ij][c]) for c in range(2))
        for ij in both
    }
    w = scale2(krauses[0], u[0])
    m = scale2(krauses[1], matmul2(u[1], w))
    into = [tuple(jnp.where(first, w[0, j][c], m[0, j][c]) for c in range(2)) for j in range(2)]
    rest = ((one, zero), (zero, zero))
    out = [tuple(jnp.where(first, u[1][i, 0][c], rest[i][c]) for c in range(2)) for i in range(2)]
    return v, m, into, out


def jumped(targets, branches, levels):
    chosen, count = [jnp.int32(-1)] * levels, jnp.int32(0)
    for layer in range(2):
        for slot in range(4):
            jump = branches[layer, slot] == 1
            for n in range(levels):
                chosen[n] = jnp.where(jnp.logical_and(jump, count == n), targets[layer, slot], chosen[n])
            count = count + jnp.where(jump, 1, 0)
    places = [16 - n for n in range(levels)]
    taken, free = {}, jnp.int32(0)
    for p in places:
        hit = [t == p for t in chosen]
        taken[p] = functools.reduce(jnp.logical_or, hit)
    result, free = [], jnp.int32(0)
    for p in places:
        other, rank = jnp.int32(-1), jnp.int32(0)
        for t in chosen:
            outside = t < 17 - levels
            other = jnp.where(jnp.logical_and(outside, rank == free), t, other)
            rank = rank + jnp.where(outside, 1, 0)
        result.append((p, jnp.where(taken[p], p, other)))
        free = free + jnp.where(taken[p], 0, 1)
    return result


def at_qubit(rows, t):
    lane = lax.broadcasted_iota(jnp.int32, rows[0][0].shape, 1)
    return [
        tuple(
            jnp.broadcast_to(jnp.sum(jnp.where(lane == t, r[c], 0.0), axis=1, keepdims=True), (1, LANES))
            for c in range(2)
        )
        for r in rows
    ]


def moved(m, places):
    lane = lax.broadcasted_iota(jnp.int32, m[0, 0][0].shape, 1)
    out = dict(m)
    for p, t in places:
        here = jnp.logical_and(lane == t, t != p)
        for ij in out:
            out[ij] = tuple(jnp.where(here, m[ij][c][:, p : p + 1], out[ij][c]) for c in range(2))
    return out


def middle_index(m, t, beta):
    bit = jnp.left_shift(jnp.int32(1), t - 14)
    clear = jnp.bitwise_and(m, jnp.bitwise_not(bit))
    return clear + (bit if beta else 0)


def part(c):
    return slice(c * LANES, (c + 1) * LANES)


def two(a, b, x, y):
    p, q = cmul(a, x), cmul(b, y)
    return p[0] + q[0], p[1] + q[1]


class Whole:
    def __init__(self, ref):
        self.ref = ref

    def rows(self, block, tile, c):
        return pl.ds(block * 256 + tile * 16 + c, 8, stride=2)

    def get(self, block, tile, c):
        return self.ref[self.rows(block, tile, c), :]

    def put(self, block, tile, c, value):
        self.ref[self.rows(block, tile, c), :] = value


class Sent(Whole):
    def __init__(self, ref, blocks):
        self.ref, self.blocks = ref, blocks

    def rows(self, block, tile, c):
        return pl.ds(tile * 16 * self.blocks + 2 * block + c, 8, stride=2 * self.blocks)


class Blocks:
    def __init__(self, ref):
        self.ref = ref

    def get(self, block, tile, c):
        return self.ref[block, pl.ds(pl.multiple_of(tile * 8, 8), 8), part(c)]

    def put(self, block, tile, c, value):
        self.ref[block, pl.ds(pl.multiple_of(tile * 8, 8), 8), part(c)] = value


def cases(t, body):
    @pl.when(t < 7)
    def _():
        body("lane", jnp.maximum(t, 0))

    @pl.when(jnp.logical_and(t >= 7, t < 10))
    def _():
        body("row", t - 7)

    @pl.when(jnp.logical_and(t >= 10, t < 14))
    def _():
        body("tile", t - 10)

    @pl.when(t >= 14)
    def _():
        body("middle", t - 14)


def over_tiles(body, unroll):
    def step(i, _):
        body(i)
        return 0

    lax.fori_loop(0, LANES // 8, step, 0, unroll=unroll)


def low_mask(axis, bit):
    index = lax.broadcasted_iota(jnp.int32, (8, LANES), axis)
    return jnp.bitwise_and(index, jnp.left_shift(jnp.int32(1), bit)) == 0


def contract(src, dst, p, t, row, unroll):
    half = 1 << (p - 14)

    def run(kind, bit):
        size = jnp.left_shift(jnp.int32(1), bit)
        axis = 1 if kind == "lane" else 0
        low = low_mask(axis, bit)
        length = LANES if kind == "lane" else 8

        def body(i):
            if kind == "tile":
                up = jnp.bitwise_and(i, size) != 0
                zero, one = jnp.bitwise_and(i, jnp.bitwise_not(size)), jnp.bitwise_or(i, size)
            for m in range(half):
                if kind == "middle":
                    shared = jnp.bitwise_and(jnp.right_shift(m, bit), 1) * half
                    k = [
                        jnp.where(t == p, m + beta * half, middle_index(m, t, beta) + shared)
                        for beta in range(2)
                    ]
                    u, w = ([src.get(n, i, c) for c in range(2)] for n in k)
                elif kind == "tile":
                    k = jnp.where(up, m + half, m)
                    u, w = ([src.get(k, at, c) for c in range(2)] for at in (zero, one))
                else:
                    u, w = [], []
                    for c in range(2):
                        a, b = src.get(m, i, c), src.get(m + half, i, c)
                        u.append(jnp.where(low, a, pltpu.roll(b, size, axis)))
                        w.append(jnp.where(low, pltpu.roll(a, length - size, axis), b))
                for c, value in enumerate(two(row[0], row[1], u, w)):
                    dst.put(m, i, c, value)

        over_tiles(body, unroll)

    cases(t, run)


def expand(src, dst, p, t, column, unroll):
    half = 1 << (p - 14)

    def run(kind, bit):
        size = jnp.left_shift(jnp.int32(1), bit)
        axis = 1 if kind == "lane" else 0
        low = low_mask(axis, bit)
        length = LANES if kind == "lane" else 8
        if kind in ("lane", "row"):
            e = tuple(jnp.where(low, column[0][c], column[1][c]) for c in range(2))

        def body(i):
            if kind == "tile":
                up = jnp.bitwise_and(i, size) != 0
                at = (jnp.bitwise_and(i, jnp.bitwise_not(size)), jnp.bitwise_or(i, size))
                ei = tuple(jnp.where(up, column[1][c], column[0][c]) for c in range(2))
            for m in range(half):
                if kind == "middle":
                    shared = jnp.bitwise_and(jnp.right_shift(m, bit), 1) * half
                    y = [src.get(m, i, c) for c in range(2)]
                    made = [
                        (jnp.where(t == p, m + beta * half, middle_index(m, t, beta) + shared), cmul(column[beta], y))
                        for beta in range(2)
                    ]
                elif kind == "tile":
                    made = [
                        (m + s * half, cmul(ei, [src.get(m, at[s], c) for c in range(2)]))
                        for s in range(2)
                    ]
                else:
                    y = [src.get(m, i, c) for c in range(2)]
                    s0 = [jnp.where(low, v, pltpu.roll(v, size, axis)) for v in y]
                    s1 = [jnp.where(low, pltpu.roll(v, length - size, axis), v) for v in y]
                    made = [(m, cmul(e, s0)), (m + half, cmul(e, s1))]
                for k, value in made:
                    for c in range(2):
                        dst.put(k, i, c, value[c])

        over_tiles(body, unroll)

    cases(t, run)


def entry(table, ij, c, qubit):
    return table[ij][c][:, qubit : qubit + 1]


def store_kron(ref, rows_ref, table, start, right, unroll):
    names = ((0, 0), (0, 1), (1, 0), (1, 1))
    for j in range(7):
        for n, ij in enumerate(names):
            for c in range(2):
                r = 8 * j + 2 * n + c
                rows_ref[r : r + 1, :] = jnp.broadcast_to(entry(table, ij, c, start + j), (1, LANES))
    step = 16

    def body(i, _):
        at = pl.multiple_of(i * step, step)
        rows = lax.broadcasted_iota(jnp.int32, (step, LANES), 0) + at
        cols = lax.broadcasted_iota(jnp.int32, (step, LANES), 1)
        if right:
            rows, cols = cols, rows
        acc = None
        for j in range(7):
            rb = jnp.bitwise_and(rows, 1 << j) == 0
            cb = jnp.bitwise_and(cols, 1 << j) == 0
            e = []
            for c in range(2):
                w = [rows_ref[8 * j + 2 * n + c : 8 * j + 2 * n + c + 1, :] for n in range(4)]
                e.append(jnp.where(rb, jnp.where(cb, w[0], w[1]), jnp.where(cb, w[2], w[3])))
            acc = tuple(e) if acc is None else cmul(acc, e)
        for n, (re, im) in enumerate(zip(split(acc[0]), split(acc[1]))):
            here, below = pl.ds(at, step), pl.ds(at + LANES, step)
            ref[n, here, :LANES] = re
            ref[n, below, LANES:] = re
            ref[n, here, LANES:] = im if right else -im
            ref[n, below, :LANES] = -im if right else im
        return 0

    lax.fori_loop(0, LANES // step, body, 0, unroll=unroll)


def mid_mix(load, store, coef, bits):
    x = [load(q) for q in range(1 << bits)]
    for j in range(bits):
        for q in range(1 << bits):
            if q >> j & 1:
                continue
            p = q | 1 << j
            x0, x1 = x[q], x[p]
            new = []
            for i in range(2):
                a, b = cmul(coef(j, i, 0), x0), cmul(coef(j, i, 1), x1)
                new.append((a[0] + b[0], a[1] + b[1]))
            x[q], x[p] = new
    for q in range(1 << bits):
        store(q, x[q])


def strided(start, stride):
    return pl.ds(start, LANES, stride=stride)


def right_stage(load, weights, tmp_ref, blocks=MID):
    for q in range(blocks):
        x = jnp.concatenate([load(q, c) for c in range(2)], 1)
        tmp_ref[q] = dot3(split(x), weights)


def left_stage(load, weights, store, blocks=MID):
    for q in range(0, blocks, 2):
        group = range(q, min(q + 2, blocks))
        ys = left_group(weights, [tuple(load(p, c) for c in range(2)) for p in group])
        for p, y in zip(group, ys):
            for c in range(2):
                store(p, c, y[c])


def mid_stage(tmp_ref, coef, bits=3, unroll=2):
    def body(i, _):
        at = pl.ds(pl.multiple_of(i * 8, 8), 8)

        def load(q):
            return tmp_ref[q, at, :LANES], tmp_ref[q, at, LANES:]

        def store(q, value):
            tmp_ref[q, at, :LANES], tmp_ref[q, at, LANES:] = value

        mid_mix(load, store, coef, bits)
        return 0

    lax.fori_loop(0, LANES // 8, body, 0, unroll=unroll)


def left_group(weights, pairs):
    x = jnp.concatenate([jnp.concatenate([a[c] for a in pairs], 1) for c in range(2)], 0)
    y = dot3(weights, split(x))
    return [
        tuple(y[c * LANES : (c + 1) * LANES, p * LANES : (p + 1) * LANES] for c in range(2))
        for p in range(len(pairs))
    ]


def level_sums(squares, mixed_ref, targets, branches, rates, layer):
    lane = lax.broadcasted_iota(jnp.int32, (LANES, LANES), 1)
    row = lax.broadcasted_iota(jnp.int32, (LANES, LANES), 0)
    weight = jnp.ones((LANES, LANES), f32)
    wq = [jnp.float32(1.0)] * MID
    out = []

    def total(v):
        return jnp.sum(jnp.sum(v, axis=0, keepdims=True), axis=1, keepdims=True)

    def mix(wq):
        mixed = wq[0] * squares[0]
        for q in range(1, MID):
            mixed = mixed + wq[q] * squares[q]
        mixed_ref[...] = mixed

    for slot in range(5):
        if slot == 0:
            mix(wq)
        else:

            @pl.when(mid)
            def _(now=tuple(wq)):
                mix(now)

        out.append(total(mixed_ref[...] * weight))
        if slot == 4:
            break
        t = targets[layer, slot]
        g = rates[layer, slot]
        jump = branches[layer, slot] == 1
        f0 = jnp.where(jump, 0.0, 1.0)
        f1 = jnp.where(jump, g, 1.0 - g)
        low, mid = t < 7, t >= 14
        index = jnp.where(low, lane, row)
        shift = jnp.where(low, t, jnp.clip(t - 7, 0, 6))
        bit = jnp.bitwise_and(jnp.right_shift(index, shift), 1)
        factor = jnp.where(bit == 1, f1, f0)
        weight = weight * jnp.where(mid, jnp.ones_like(factor), factor)
        tm = jnp.where(mid, t - 14, 0)
        wq = [
            w * jnp.where(mid, jnp.where(jnp.bitwise_and(jnp.right_shift(q, tm), 1) == 1, f1, f0), 1.0)
            for q, w in enumerate(wq)
        ]
    return out, weight, wq


def prep_kernel(x_hbm, angles_ref, targets, branches, rates, g_ref, sums_ref,
                tmp_ref, rows_ref, low_v_ref, top_v_ref, squares_ref, mixed_ref,
                x_ref, sem, *, unroll):
    copy = pltpu.make_async_copy(x_hbm, x_ref, sem)
    copy.start()
    v, m, _, _ = tables(angles_ref, targets, branches, rates)
    store_kron(g_ref, rows_ref, m, 17, False, min(unroll, 8))
    store_kron(low_v_ref, rows_ref, v, 0, True, min(unroll, 8))
    store_kron(top_v_ref, rows_ref, v, 7, False, min(unroll, 8))
    v_low, v_top = ((r[0], r[1]) for r in (low_v_ref, top_v_ref))
    copy.wait()
    right_stage(lambda q, c: x_ref[strided(q * 256 + c, 2), :], v_low, tmp_ref)
    v_mid = {
        (j, i, k, c): jnp.broadcast_to(entry(v, (i, k), c, 14 + j), (8, LANES))
        for j in range(3) for i in range(2) for k in range(2) for c in range(2)
    }
    mid_stage(tmp_ref, lambda j, i, k: (v_mid[j, i, k, 0], v_mid[j, i, k, 1]), 3, unroll)

    def keep(p, c, value):
        tmp_ref[p, :, part(c)] = value

    left_stage(lambda p, c: tmp_ref[p, :, part(c)], v_top, keep)
    for q in range(MID):
        re, im = (tmp_ref[q, :, part(c)] for c in range(2))
        squares_ref[q] = re * re + im * im
    first, weight, wq = level_sums(squares_ref, mixed_ref, targets, branches, rates, 0)
    kept = first[4]
    alpha = jnp.where(kept > 0.0, lax.rsqrt(jnp.maximum(kept, 1e-37)), 0.0)
    root = jnp.sqrt(weight)
    for q in range(MID):
        r = root * jnp.sqrt(jnp.full((1, LANES), wq[q], f32)) * alpha
        re, im = (tmp_ref[q, :, part(c)] * r for c in range(2))
        squares_ref[q] = re * re + im * im
    second, _, _ = level_sums(squares_ref, mixed_ref, targets, branches, rates, 1)
    base = jnp.where(second[0] > 0.0, second[0], 1.0)
    values = first + [s / base for s in second[1:]]
    lane = lax.broadcasted_iota(jnp.int32, (8, LANES), 1)
    packed = jnp.zeros((8, LANES), f32)
    for k, s in enumerate(values):
        packed = jnp.where(lane == k, s, packed)
    sums_ref[...] = packed


def tables_kernel(after_ref, angles_ref, targets, branches, rates, low_ref, top_ref, mid_ref, rows_ref, *, levels, unroll):
    _, m, _, out = tables(angles_ref, targets, branches, rates)
    places = jumped(targets, branches, levels)
    for n, (_, t) in enumerate(places):
        e = at_qubit(out, t)
        for i in range(2):
            for c in range(2):
                r = 24 + 4 * n + 2 * i + c
                mid_ref[r : r + 1, :] = e[i][c]
    m = moved(m, places)
    store_kron(low_ref, rows_ref, m, 0, True, unroll)
    store_kron(top_ref, rows_ref, m, 7, False, unroll)
    for j in range(3):
        for i in range(2):
            for k in range(2):
                for c in range(2):
                    r = ((j * 2 + i) * 2 + k) * 2 + c
                    mid_ref[r : r + 1, :] = jnp.broadcast_to(
                        entry(m, (i, k), c, 14 + j), (1, LANES)
                    )


def contract_kernel(x_ref, angles_ref, targets, branches, rates, out_ref, *refs, levels, count):
    spare = list(refs)
    if count:
        count_ref = spare.pop(0)
        jumps = jnp.int32(0)
        for layer in range(2):
            for slot in range(4):
                jumps = jumps + jnp.where(branches[layer, slot] == 1, 1, 0)
        count_ref[0] = jnp.minimum(jumps, levels)
    _, _, into, _ = tables(angles_ref, targets, branches, rates)
    places = jumped(targets, branches, levels)
    rows = [at_qubit(into, t) for _, t in places]
    src = Whole(x_ref)
    for n, (p, t) in enumerate(places):
        dst = Sent(out_ref, MID >> levels) if n == levels - 1 else Blocks(spare[n])
        contract(src, dst, p, t, rows[n], 8 if count else 2)
        src = dst


def global_kernel(x_ref, g_ref, sums_ref, out_ref, token_ref, *, blocks):
    token_ref[...] = sums_ref[...]
    stride = 2 * blocks + 1

    def store(p, c, value):
        out_ref[strided(2 * p + c, stride), :] = value

    left_stage(
        lambda p, c: x_ref[strided(2 * p + c, 2 * blocks), :], (g_ref[0], g_ref[1]), store, blocks
    )
    out_ref[strided(2 * blocks, stride), :] = jnp.broadcast_to(
        sums_ref[0:1, :], (LANES, LANES)
    )


def final_kernel(x_ref, low_ref, top_ref, mid_ref, targets, branches,
                 out_ref, weights_ref, tmp_ref, other_ref, *, levels, whole):
    blocks = MID >> levels
    stride = 2 * blocks + 1
    parts = x_ref[strided(2 * blocks, stride), :]
    totals = jnp.sum(parts, axis=0, keepdims=True)
    kept = parts[:, 4:5]
    kept_total = jnp.maximum(totals[:, 4:5], 1e-37)
    ratios = jnp.sum(parts * (kept / kept_total), axis=0, keepdims=True)
    lane = lax.broadcasted_iota(jnp.int32, (1, LANES), 1)
    row = jnp.zeros((1, LANES), f32)
    factors = []
    mean = [totals[:, k : k + 1] / whole for k in range(5)]
    for layer in range(2):
        factor = jnp.ones((1, 1), f32)
        for slot in range(4):
            before = mean[slot] * factor * factor
            after = mean[slot + 1] * factor * factor
            row = jnp.where(lane == layer * 4 + slot, after / before, row)
            factor = factor * lax.rsqrt(after + EPS)
        factors.append(factor)
        if layer == 0:
            start = mean[4] * factor * factor
            mean = [start] + [start * ratios[:, 5 + k : 6 + k] for k in range(4)]
    weights_ref[0:1, :] = row[:, 0:4]
    weights_ref[1:2, :] = row[:, 4:8]

    def load(q, c):
        if levels:
            return x_ref[strided(2 * q + c, stride), :]
        return jnp.concatenate(
            [x_ref[pl.ds((q * 16 + k) * stride + c, 8, stride=2), :] for k in range(16)], 0
        )

    right_stage(load, (low_ref[0], low_ref[1]), tmp_ref, blocks)

    def coef(j, i, k):
        r = ((j * 2 + i) * 2 + k) * 2
        return mid_ref[r : r + 1, :], mid_ref[r + 1 : r + 2, :]

    if levels < 3:
        mid_stage(tmp_ref, coef, 3 - levels)

    def store(q, c, value):
        value = value * factors[0] * factors[1]
        if levels:
            tmp_ref[q, :, part(c)] = value
        else:
            out_ref[strided(q * 256 + c, 2), :] = value

    left_stage(lambda q, c: tmp_ref[q, :, part(c)], (top_ref[0], top_ref[1]), store, blocks)
    src, spare = Blocks(tmp_ref), [other_ref, tmp_ref]
    for n, (p, t) in reversed(list(enumerate(jumped(targets, branches, levels)))):
        r = 24 + 4 * n
        column = [
            tuple(mid_ref[r + 2 * i + c : r + 2 * i + c + 1, :] for c in range(2)) for i in range(2)
        ]
        dst = Whole(out_ref) if n == 0 else Blocks(spare[(levels - 1 - n) % 2])
        expand(src, dst, p, t, column, 8 if levels == 3 else 2)
        src = dst


def cost(flops):
    return pl.CostEstimate(flops=flops, bytes_accessed=2_000_000, transcendentals=0)


def local_rows(initial_state):
    return initial_state.reshape(2, -1, LANES).transpose(1, 0, 2).reshape(-1, LANES)


def contracted(levels, count, x, *settings):
    vmem, smem = (pl.BlockSpec(memory_space=m) for m in (pltpu.VMEM, pltpu.SMEM))
    tmp = pltpu.VMEM((MID, LANES, 2 * LANES), f32)
    out = pltpu.VMEM((x.shape[0] >> levels, LANES), f32)
    return pl.pallas_call(
        functools.partial(contract_kernel, levels=levels, count=count),
        out_shape=(out, jax.ShapeDtypeStruct((1,), jnp.int32)) if count else out,
        in_specs=[vmem, vmem, smem, smem, smem],
        out_specs=(vmem, smem) if count else vmem,
        scratch_shapes=[tmp] * (levels - 1),
        compiler_params=pltpu.CompilerParams(vmem_limit_bytes=24 << 20),
        cost_estimate=cost(20_000_000),
        name=f"contract_{levels}",
    )(x, *settings)


def program(levels, ready, initial_state, gate_angles, damp_qubits, kraus_branch, damping):
    devices = lax.axis_size(AXES)
    local = initial_state.shape[1]
    whole = float(local * devices)
    rows = local * 2 // LANES
    blocks = MID >> levels
    vmem = pl.BlockSpec(memory_space=pltpu.VMEM)
    smem = pl.BlockSpec(memory_space=pltpu.SMEM)
    big = pltpu.VMEM((2, 256, 256), bf16)
    tmp = pltpu.VMEM((MID, LANES, 2 * LANES), f32)
    near = functools.partial(pltpu.with_memory_space_constraint, memory_space=pltpu.VMEM)
    params = pltpu.CompilerParams(vmem_limit_bytes=24 << 20)
    x = local_rows(initial_state)
    settings = (gate_angles.transpose(1, 0, 2), damp_qubits, kraus_branch, damping)
    table = pltpu.VMEM((2, 256, 256), bf16)
    in_specs = [vmem, vmem, smem, smem, smem]
    sent = x
    if levels:
        sent = ready if levels == 3 else contracted(levels, False, near(x), *settings)
    sent = sent.reshape((devices, 1, 2 * blocks * LANES) if levels > 1 else (devices, 2 * blocks, LANES))
    swapped = lax.all_to_all(sent, AXES, split_axis=0, concat_axis=0, tiled=True)
    unroll = 4 if levels == 3 else 1
    g, sums = pl.pallas_call(
        functools.partial(prep_kernel, unroll=unroll),
        out_shape=(big, pltpu.VMEM((8, LANES), f32)),
        in_specs=[pl.BlockSpec(memory_space=pl.ANY)] + in_specs[1:],
        out_specs=(vmem,) * 2,
        scratch_shapes=[tmp, pltpu.VMEM((56, LANES), f32), table, table,
                        pltpu.VMEM((MID, LANES, LANES), f32), pltpu.VMEM((LANES, LANES), f32),
                        pltpu.VMEM((rows, LANES), f32), pltpu.SemaphoreType.DMA],
        compiler_params=params,
        cost_estimate=cost(2_000_000_000),
        name=f"prep_{levels}",
    )(x, *settings)
    mixed, token = pl.pallas_call(
        functools.partial(global_kernel, blocks=blocks),
        out_shape=(pltpu.VMEM((devices * (2 * blocks + 1), LANES), f32), pltpu.VMEM((8, LANES), f32)),
        in_specs=[vmem] * 3,
        out_specs=(vmem,) * 2,
        compiler_params=params,
        cost_estimate=cost(400_000_000 >> levels),
        name=f"global_gates_{levels}",
    )(near(swapped.reshape(rows >> levels, LANES)), near(g), near(sums))
    back = lax.all_to_all(
        mixed.reshape(devices, 1, (2 * blocks + 1) * LANES), AXES, split_axis=0, concat_axis=0, tiled=True
    )
    low, top, mid = pl.pallas_call(
        functools.partial(tables_kernel, levels=levels, unroll=2),
        out_shape=(big, big, pltpu.VMEM((40, LANES), f32)),
        in_specs=in_specs,
        out_specs=(vmem,) * 3,
        scratch_shapes=[pltpu.VMEM((56, LANES), f32)],
        compiler_params=params,
        cost_estimate=cost(1_000_000_000),
        name=f"tables_{levels}",
    )(near(token), *settings)
    out, weights = pl.pallas_call(
        functools.partial(final_kernel, levels=levels, whole=whole),
        out_shape=(jax.ShapeDtypeStruct((rows, LANES), f32),
                   jax.ShapeDtypeStruct(damp_qubits.shape, f32)),
        in_specs=[vmem] * 4 + [smem] * 2,
        out_specs=(vmem, vmem),
        scratch_shapes=[tmp, tmp],
        compiler_params=params,
        cost_estimate=cost(800_000_000),
        name=f"local_gates_{levels}",
    )(near(back.reshape(devices * (2 * blocks + 1), LANES)), near(low), near(top), near(mid),
      damp_qubits, kraus_branch)
    out = out.reshape(rows // 2, 2, LANES).transpose(1, 0, 2).reshape(2, local)
    return out, weights


def on_device(*args):
    initial_state, gate_angles, *rest = args
    ready, levels = contracted(
        3, True, local_rows(initial_state), gate_angles.transpose(1, 0, 2), *rest
    )
    return lax.switch(levels[0], [functools.partial(program, n) for n in range(4)], ready, *args)


def solution(mesh):
    return jax.shard_map(
        on_device,
        mesh=mesh,
        in_specs=(P(None, AXES), P(), P(), P(), P()),
        out_specs=(P(None, AXES), P()),
        check_vma=False,
    )
```

```python
import functools

import jax
import jax.numpy as jnp
from jax import lax
from jax.experimental import pallas as pl
from jax.experimental.pallas import tpu as pltpu
from jax.sharding import PartitionSpec as P

AXES = ("hi", "lo")
EPS = 1e-6
LANES = 128
ROWS = 16
MID = 8
f32 = jnp.float32
bf16 = jnp.bfloat16


def split(x):
    hi = x.astype(bf16)
    return hi, (x - hi.astype(f32)).astype(bf16)


def dot3(a, b):
    (ah, al), (bh, bl) = a, b
    return jnp.dot(
        jnp.concatenate([ah, ah, al], 1),
        jnp.concatenate([bh, bl, bh], 0),
        preferred_element_type=f32,
    )


def cmul(a, b):
    return a[0] * b[0] - a[1] * b[1], a[0] * b[1] + a[1] * b[0]


def matmul2(a, b):
    out = {}
    for i in range(2):
        for j in range(2):
            p, q = cmul(a[i, 0], b[0, j]), cmul(a[i, 1], b[1, j])
            out[i, j] = (p[0] + q[0], p[1] + q[1])
    return out


def scale2(k, u):
    k00, k01, k11 = k
    out = {}
    for j in range(2):
        out[0, j] = tuple(k00 * u[0, j][c] + k01 * u[1, j][c] for c in range(2))
        out[1, j] = tuple(k11 * u[1, j][c] for c in range(2))
    return out


def gates(angles_ref):
    a, b, c = (angles_ref[k] for k in range(3))
    half = jnp.concatenate([b, a + c, a - c], 0) * 0.5
    cosine, sine = jnp.cos(half), jnp.sin(half)
    out = []
    for layer in range(2):
        co, cs, cd = (cosine[2 * k + layer : 2 * k + layer + 1] for k in range(3))
        si, ss, sd = (sine[2 * k + layer : 2 * k + layer + 1] for k in range(3))
        out.append({
            (0, 0): (cs * co, -ss * co),
            (0, 1): (-cd * si, sd * si),
            (1, 0): (cd * si, sd * si),
            (1, 1): (cs * co, ss * co),
        })
    return out


def tables(angles_ref, targets, branches, rates):
    qubits = angles_ref.shape[2]
    lane = lax.broadcasted_iota(jnp.int32, (1, qubits), 1)
    one, zero = jnp.ones((1, qubits), f32), jnp.zeros((1, qubits), f32)
    u = gates(angles_ref)
    krauses, first = [], zero > 1.0
    for layer in range(2):
        k00, k01, k11 = one, zero, one
        for slot in range(4):
            here = lane == targets[layer, slot]
            jump = branches[layer, slot] == 1
            g = jnp.full((1, qubits), rates[layer, slot], f32)
            k00 = jnp.where(here, jnp.where(jump, 0.0, 1.0), k00)
            k01 = jnp.where(here, jnp.where(jump, jnp.sqrt(g), 0.0), k01)
            k11 = jnp.where(here, jnp.where(jump, 0.0, jnp.sqrt(1.0 - g)), k11)
            if layer == 0:
                first = jnp.logical_or(first, here)
        krauses.append((k00, k01, k11))
    both = matmul2(u[1], u[0])
    v = {
        ij: tuple(jnp.where(first, u[0][ij][c], both[ij][c]) for c in range(2))
        for ij in both
    }
    w = scale2(krauses[0], u[0])
    m = scale2(krauses[1], matmul2(u[1], w))
    into = [tuple(jnp.where(first, w[0, j][c], m[0, j][c]) for c in range(2)) for j in range(2)]
    rest = ((one, zero), (zero, zero))
    out = [tuple(jnp.where(first, u[1][i, 0][c], rest[i][c]) for c in range(2)) for i in range(2)]
    return v, m, into, out


def jumped(targets, branches, levels):
    chosen, count = [jnp.int32(-1)] * levels, jnp.int32(0)
    for layer in range(2):
        for slot in range(4):
            jump = branches[layer, slot] == 1
            for n in range(levels):
                chosen[n] = jnp.where(jnp.logical_and(jump, count == n), targets[layer, slot], chosen[n])
            count = count + jnp.where(jump, 1, 0)
    places = [16 - n for n in range(levels)]
    taken, free = {}, jnp.int32(0)
    for p in places:
        hit = [t == p for t in chosen]
        taken[p] = functools.reduce(jnp.logical_or, hit)
    result, free = [], jnp.int32(0)
    for p in places:
        other, rank = jnp.int32(-1), jnp.int32(0)
        for t in chosen:
            outside = t < 17 - levels
            other = jnp.where(jnp.logical_and(outside, rank == free), t, other)
            rank = rank + jnp.where(outside, 1, 0)
        result.append((p, jnp.where(taken[p], p, other)))
        free = free + jnp.where(taken[p], 0, 1)
    return result


def at_qubit(rows, t):
    lane = lax.broadcasted_iota(jnp.int32, rows[0][0].shape, 1)
    return [
        tuple(
            jnp.broadcast_to(jnp.sum(jnp.where(lane == t, r[c], 0.0), axis=1, keepdims=True), (1, LANES))
            for c in range(2)
        )
        for r in rows
    ]


def moved(m, places):
    lane = lax.broadcasted_iota(jnp.int32, m[0, 0][0].shape, 1)
    out = dict(m)
    for p, t in places:
        here = jnp.logical_and(lane == t, t != p)
        for ij in out:
            out[ij] = tuple(jnp.where(here, m[ij][c][:, p : p + 1], out[ij][c]) for c in range(2))
    return out


def middle_index(m, t, beta):
    bit = jnp.left_shift(jnp.int32(1), t - 14)
    clear = jnp.bitwise_and(m, jnp.bitwise_not(bit))
    return clear + (bit if beta else 0)


def part(c):
    return slice(c * LANES, (c + 1) * LANES)


def two(a, b, x, y):
    p, q = cmul(a, x), cmul(b, y)
    return p[0] + q[0], p[1] + q[1]


class Whole:
    def __init__(self, ref):
        self.ref = ref

    def rows(self, block, tile, c):
        return pl.ds(block * 256 + tile * 16 + c, 8, stride=2)

    def get(self, block, tile, c):
        return self.ref[self.rows(block, tile, c), :]

    def put(self, block, tile, c, value):
        self.ref[self.rows(block, tile, c), :] = value


class Sent(Whole):
    def __init__(self, ref, blocks):
        self.ref, self.blocks = ref, blocks

    def rows(self, block, tile, c):
        return pl.ds(tile * 16 * self.blocks + 2 * block + c, 8, stride=2 * self.blocks)


class Blocks:
    def __init__(self, ref):
        self.ref = ref

    def get(self, block, tile, c):
        return self.ref[block, pl.ds(pl.multiple_of(tile * 8, 8), 8), part(c)]

    def put(self, block, tile, c, value):
        self.ref[block, pl.ds(pl.multiple_of(tile * 8, 8), 8), part(c)] = value


def cases(t, body):
    @pl.when(t < 7)
    def _():
        body("lane", jnp.maximum(t, 0))

    @pl.when(jnp.logical_and(t >= 7, t < 10))
    def _():
        body("row", t - 7)

    @pl.when(jnp.logical_and(t >= 10, t < 14))
    def _():
        body("tile", t - 10)

    @pl.when(t >= 14)
    def _():
        body("middle", t - 14)


def over_tiles(body, unroll):
    def step(i, _):
        body(i)
        return 0

    lax.fori_loop(0, LANES // 8, step, 0, unroll=unroll)


def low_mask(axis, bit):
    index = lax.broadcasted_iota(jnp.int32, (8, LANES), axis)
    return jnp.bitwise_and(index, jnp.left_shift(jnp.int32(1), bit)) == 0


def contract(src, dst, p, t, row, unroll):
    half = 1 << (p - 14)

    def run(kind, bit):
        size = jnp.left_shift(jnp.int32(1), bit)
        axis = 1 if kind == "lane" else 0
        low = low_mask(axis, bit)
        length = LANES if kind == "lane" else 8

        def body(i):
            if kind == "tile":
                up = jnp.bitwise_and(i, size) != 0
                zero, one = jnp.bitwise_and(i, jnp.bitwise_not(size)), jnp.bitwise_or(i, size)
            for m in range(half):
                if kind == "middle":
                    shared = jnp.bitwise_and(jnp.right_shift(m, bit), 1) * half
                    k = [
                        jnp.where(t == p, m + beta * half, middle_index(m, t, beta) + shared)
                        for beta in range(2)
                    ]
                    u, w = ([src.get(n, i, c) for c in range(2)] for n in k)
                elif kind == "tile":
                    k = jnp.where(up, m + half, m)
                    u, w = ([src.get(k, at, c) for c in range(2)] for at in (zero, one))
                else:
                    u, w = [], []
                    for c in range(2):
                        a, b = src.get(m, i, c), src.get(m + half, i, c)
                        u.append(jnp.where(low, a, pltpu.roll(b, size, axis)))
                        w.append(jnp.where(low, pltpu.roll(a, length - size, axis), b))
                for c, value in enumerate(two(row[0], row[1], u, w)):
                    dst.put(m, i, c, value)

        over_tiles(body, unroll)

    cases(t, run)


def expand(src, dst, p, t, column, unroll):
    half = 1 << (p - 14)

    def run(kind, bit):
        size = jnp.left_shift(jnp.int32(1), bit)
        axis = 1 if kind == "lane" else 0
        low = low_mask(axis, bit)
        length = LANES if kind == "lane" else 8
        if kind in ("lane", "row"):
            e = tuple(jnp.where(low, column[0][c], column[1][c]) for c in range(2))

        def body(i):
            if kind == "tile":
                up = jnp.bitwise_and(i, size) != 0
                at = (jnp.bitwise_and(i, jnp.bitwise_not(size)), jnp.bitwise_or(i, size))
                ei = tuple(jnp.where(up, column[1][c], column[0][c]) for c in range(2))
            for m in range(half):
                if kind == "middle":
                    shared = jnp.bitwise_and(jnp.right_shift(m, bit), 1) * half
                    y = [src.get(m, i, c) for c in range(2)]
                    made = [
                        (jnp.where(t == p, m + beta * half, middle_index(m, t, beta) + shared), cmul(column[beta], y))
                        for beta in range(2)
                    ]
                elif kind == "tile":
                    made = [
                        (m + s * half, cmul(ei, [src.get(m, at[s], c) for c in range(2)]))
                        for s in range(2)
                    ]
                else:
                    y = [src.get(m, i, c) for c in range(2)]
                    s0 = [jnp.where(low, v, pltpu.roll(v, size, axis)) for v in y]
                    s1 = [jnp.where(low, pltpu.roll(v, length - size, axis), v) for v in y]
                    made = [(m, cmul(e, s0)), (m + half, cmul(e, s1))]
                for k, value in made:
                    for c in range(2):
                        dst.put(k, i, c, value[c])

        over_tiles(body, unroll)

    cases(t, run)


def entry(table, ij, c, qubit):
    return table[ij][c][:, qubit : qubit + 1]


def store_kron(ref, rows_ref, table, start, right, unroll):
    names = ((0, 0), (0, 1), (1, 0), (1, 1))
    for j in range(7):
        for n, ij in enumerate(names):
            for c in range(2):
                r = 8 * j + 2 * n + c
                rows_ref[r : r + 1, :] = jnp.broadcast_to(entry(table, ij, c, start + j), (1, LANES))
    step = 16

    def row(j, n, c):
        r = 8 * j + 2 * n + c
        return rows_ref[r : r + 1, :]

    rows = lax.broadcasted_iota(jnp.int32, (step, LANES), 0)
    cols = lax.broadcasted_iota(jnp.int32, (step, LANES), 1)
    if right:
        rows, cols = cols, rows
    shared = None
    for j in range(4):
        rb = jnp.bitwise_and(rows, 1 << j) == 0
        cb = jnp.bitwise_and(cols, 1 << j) == 0
        e = tuple(
            jnp.where(rb, jnp.where(cb, row(j, 0, c), row(j, 1, c)), jnp.where(cb, row(j, 2, c), row(j, 3, c)))
            for c in range(2)
        )
        shared = e if shared is None else cmul(shared, e)
    lane = lax.broadcasted_iota(jnp.int32, (1, LANES), 1)

    def body(i, _):
        at = pl.multiple_of(i * step, step)
        own = None
        for j in range(4, 7):
            zero = jnp.bitwise_and(jnp.right_shift(i, j - 4), 1) == 0
            first = jnp.bitwise_and(lane, 1 << j) == 0
            e = []
            for c in range(2):
                w = [row(j, n, c) for n in range(4)]
                a = jnp.where(zero, w[0], w[1] if right else w[2])
                b = jnp.where(zero, w[2] if right else w[1], w[3])
                e.append(jnp.where(first, a, b))
            own = tuple(e) if own is None else cmul(own, e)
        acc = cmul(shared, own)
        for n, (re, im) in enumerate(zip(split(acc[0]), split(acc[1]))):
            here, below = pl.ds(at, step), pl.ds(at + LANES, step)
            ref[n, here, :LANES] = re
            ref[n, below, LANES:] = re
            ref[n, here, LANES:] = im if right else -im
            ref[n, below, :LANES] = -im if right else im
        return 0

    lax.fori_loop(0, LANES // step, body, 0, unroll=unroll)


def mid_mix(load, store, coef, bits, blocks):
    x = [load(q) for q in range(blocks)]
    for j in bits:
        for q in range(blocks):
            if q >> j & 1:
                continue
            p = q | 1 << j
            x0, x1 = x[q], x[p]
            new = []
            for i in range(2):
                a, b = cmul(coef(j, i, 0), x0), cmul(coef(j, i, 1), x1)
                new.append((a[0] + b[0], a[1] + b[1]))
            x[q], x[p] = new
    for q in range(blocks):
        store(q, x[q])


def strided(start, stride):
    return pl.ds(start, LANES, stride=stride)


def right_stage(load, weights, tmp_ref, blocks=MID):
    for q in range(blocks):
        x = jnp.concatenate([load(q, c) for c in range(2)], 1)
        tmp_ref[q] = dot3(split(x), weights)


def left_stage(load, weights, store, blocks=MID):
    for q in range(0, blocks, 2):
        group = range(q, min(q + 2, blocks))
        ys = left_group(weights, [tuple(load(p, c) for c in range(2)) for p in group])
        for p, y in zip(group, ys):
            for c in range(2):
                store(p, c, y[c])


def mid_stage(tmp_ref, coef, bits, blocks, unroll):
    def body(i, _):
        at = pl.ds(pl.multiple_of(i * 8, 8), 8)

        def load(q):
            return tmp_ref[q, at, :LANES], tmp_ref[q, at, LANES:]

        def store(q, value):
            tmp_ref[q, at, :LANES], tmp_ref[q, at, LANES:] = value

        mid_mix(load, store, coef, bits, blocks)
        return 0

    lax.fori_loop(0, LANES // 8, body, 0, unroll=unroll)


def left_group(weights, pairs):
    x = jnp.concatenate([jnp.concatenate([a[c] for a in pairs], 1) for c in range(2)], 0)
    y = dot3(weights, split(x))
    return [
        tuple(y[c * LANES : (c + 1) * LANES, p * LANES : (p + 1) * LANES] for c in range(2))
        for p in range(len(pairs))
    ]


def level_sums(squares, mixed_ref, targets, branches, rates, layer):
    lane = lax.broadcasted_iota(jnp.int32, (LANES, LANES), 1)
    row = lax.broadcasted_iota(jnp.int32, (LANES, LANES), 0)
    weight = jnp.ones((LANES, LANES), f32)
    wq = [jnp.float32(1.0)] * MID
    out = []

    def total(v):
        return jnp.sum(jnp.sum(v, axis=0, keepdims=True), axis=1, keepdims=True)

    def mix(wq):
        mixed = wq[0] * squares[0]
        for q in range(1, MID):
            mixed = mixed + wq[q] * squares[q]
        mixed_ref[...] = mixed

    for slot in range(5):
        if slot == 0:
            mix(wq)
        else:

            @pl.when(mid)
            def _(now=tuple(wq)):
                mix(now)

        out.append(total(mixed_ref[...] * weight))
        if slot == 4:
            break
        t = targets[layer, slot]
        g = rates[layer, slot]
        jump = branches[layer, slot] == 1
        f0 = jnp.where(jump, 0.0, 1.0)
        f1 = jnp.where(jump, g, 1.0 - g)
        low, mid = t < 7, t >= 14
        index = jnp.where(low, lane, row)
        shift = jnp.where(low, t, jnp.clip(t - 7, 0, 6))
        bit = jnp.bitwise_and(jnp.right_shift(index, shift), 1)
        factor = jnp.where(bit == 1, f1, f0)
        weight = weight * jnp.where(mid, jnp.ones_like(factor), factor)
        tm = jnp.where(mid, t - 14, 0)
        wq = [
            w * jnp.where(mid, jnp.where(jnp.bitwise_and(jnp.right_shift(q, tm), 1) == 1, f1, f0), 1.0)
            for q, w in enumerate(wq)
        ]
    return out, weight, wq


def prep_kernel(x_hbm, angles_ref, targets, branches, rates, g_ref, sums_ref,
                tmp_ref, rows_ref, low_v_ref, top_v_ref, squares_ref, mixed_ref,
                x_ref, sem, *, unroll):
    copy = pltpu.make_async_copy(x_hbm, x_ref, sem)
    copy.start()
    v, m, _, _ = tables(angles_ref, targets, branches, rates)
    store_kron(g_ref, rows_ref, m, 17, False, min(unroll, 8))
    store_kron(low_v_ref, rows_ref, v, 0, True, min(unroll, 8))
    store_kron(top_v_ref, rows_ref, v, 7, False, min(unroll, 8))
    v_low, v_top = ((r[0], r[1]) for r in (low_v_ref, top_v_ref))
    copy.wait()
    right_stage(lambda q, c: x_ref[strided(q * 256 + c, 2), :], v_low, tmp_ref)
    v_mid = {
        (j, i, k, c): jnp.broadcast_to(entry(v, (i, k), c, 14 + j), (8, LANES))
        for j in range(3) for i in range(2) for k in range(2) for c in range(2)
    }
    for bit in range(3):
        hits = [targets[layer, slot] == 14 + bit for layer in range(2) for slot in range(4)]

        @pl.when(functools.reduce(jnp.logical_or, hits))
        def _(bit=bit):
            mid_stage(
                tmp_ref, lambda j, i, k: (v_mid[j, i, k, 0], v_mid[j, i, k, 1]), [bit], MID, unroll
            )


    def keep(p, c, value):
        tmp_ref[p, :, part(c)] = value

    left_stage(lambda p, c: tmp_ref[p, :, part(c)], v_top, keep)
    for q in range(MID):
        re, im = (tmp_ref[q, :, part(c)] for c in range(2))
        squares_ref[q] = re * re + im * im
    first, weight, wq = level_sums(squares_ref, mixed_ref, targets, branches, rates, 0)
    kept = first[4]
    alpha = jnp.where(kept > 0.0, lax.rsqrt(jnp.maximum(kept, 1e-37)), 0.0)
    root = jnp.sqrt(weight)
    for q in range(MID):
        r = root * jnp.sqrt(jnp.full((1, LANES), wq[q], f32)) * alpha
        re, im = (tmp_ref[q, :, part(c)] * r for c in range(2))
        squares_ref[q] = re * re + im * im
    second, _, _ = level_sums(squares_ref, mixed_ref, targets, branches, rates, 1)
    base = jnp.where(second[0] > 0.0, second[0], 1.0)
    values = first + [s / base for s in second[1:]]
    lane = lax.broadcasted_iota(jnp.int32, (8, LANES), 1)
    packed = jnp.zeros((8, LANES), f32)
    for k, s in enumerate(values):
        packed = jnp.where(lane == k, s, packed)
    sums_ref[...] = packed


def tables_kernel(after_ref, angles_ref, targets, branches, rates, low_ref, top_ref, mid_ref, rows_ref, *, levels, unroll):
    _, m, _, out = tables(angles_ref, targets, branches, rates)
    places = jumped(targets, branches, levels)
    for n, (_, t) in enumerate(places):
        e = at_qubit(out, t)
        for i in range(2):
            for c in range(2):
                r = 24 + 4 * n + 2 * i + c
                mid_ref[r : r + 1, :] = e[i][c]
    m = moved(m, places)
    store_kron(low_ref, rows_ref, m, 0, True, unroll)
    store_kron(top_ref, rows_ref, m, 7, False, unroll)
    for j in range(3):
        for i in range(2):
            for k in range(2):
                for c in range(2):
                    r = ((j * 2 + i) * 2 + k) * 2 + c
                    mid_ref[r : r + 1, :] = jnp.broadcast_to(
                        entry(m, (i, k), c, 14 + j), (1, LANES)
                    )


def contract_kernel(x_ref, angles_ref, targets, branches, rates, out_ref, *refs, levels, count):
    spare = list(refs)
    if count:
        count_ref = spare.pop(0)
        jumps = jnp.int32(0)
        for layer in range(2):
            for slot in range(4):
                jumps = jumps + jnp.where(branches[layer, slot] == 1, 1, 0)
        count_ref[0] = jnp.minimum(jumps, levels)
    _, _, into, _ = tables(angles_ref, targets, branches, rates)
    places = jumped(targets, branches, levels)
    rows = [at_qubit(into, t) for _, t in places]
    src = Whole(x_ref)
    for n, (p, t) in enumerate(places):
        dst = Sent(out_ref, MID >> levels) if n == levels - 1 else Blocks(spare[n])
        contract(src, dst, p, t, rows[n], 8 if count else 2)
        src = dst


def global_kernel(x_ref, g_ref, sums_ref, out_ref, token_ref, *, blocks):
    token_ref[...] = sums_ref[...]
    stride = 2 * blocks + 1

    def store(p, c, value):
        out_ref[strided(2 * p + c, stride), :] = value

    left_stage(
        lambda p, c: x_ref[strided(2 * p + c, 2 * blocks), :], (g_ref[0], g_ref[1]), store, blocks
    )
    out_ref[strided(2 * blocks, stride), :] = jnp.broadcast_to(
        sums_ref[0:1, :], (LANES, LANES)
    )


def final_kernel(x_ref, low_ref, top_ref, mid_ref, targets, branches,
                 out_ref, weights_ref, tmp_ref, other_ref, *, levels, whole):
    blocks = MID >> levels
    stride = 2 * blocks + 1
    parts = x_ref[strided(2 * blocks, stride), :]
    totals = jnp.sum(parts, axis=0, keepdims=True)
    kept = parts[:, 4:5]
    kept_total = jnp.maximum(totals[:, 4:5], 1e-37)
    ratios = jnp.sum(parts * (kept / kept_total), axis=0, keepdims=True)
    lane = lax.broadcasted_iota(jnp.int32, (1, LANES), 1)
    row = jnp.zeros((1, LANES), f32)
    factors = []
    mean = [totals[:, k : k + 1] / whole for k in range(5)]
    for layer in range(2):
        factor = jnp.ones((1, 1), f32)
        for slot in range(4):
            before = mean[slot] * factor * factor
            after = mean[slot + 1] * factor * factor
            row = jnp.where(lane == layer * 4 + slot, after / before, row)
            factor = factor * lax.rsqrt(after + EPS)
        factors.append(factor)
        if layer == 0:
            start = mean[4] * factor * factor
            mean = [start] + [start * ratios[:, 5 + k : 6 + k] for k in range(4)]
    weights_ref[0:1, :] = row[:, 0:4]
    weights_ref[1:2, :] = row[:, 4:8]

    def load(q, c):
        if levels:
            return x_ref[strided(2 * q + c, stride), :]
        return jnp.concatenate(
            [x_ref[pl.ds((q * 16 + k) * stride + c, 8, stride=2), :] for k in range(16)], 0
        )

    right_stage(load, (low_ref[0], low_ref[1]), tmp_ref, blocks)

    def coef(j, i, k):
        r = ((j * 2 + i) * 2 + k) * 2
        return mid_ref[r : r + 1, :], mid_ref[r + 1 : r + 2, :]

    if levels < 3:
        mid_stage(tmp_ref, coef, range(3 - levels), blocks, 2)

    def store(q, c, value):
        value = value * factors[0] * factors[1]
        if levels:
            tmp_ref[q, :, part(c)] = value
        else:
            out_ref[strided(q * 256 + c, 2), :] = value

    left_stage(lambda q, c: tmp_ref[q, :, part(c)], (top_ref[0], top_ref[1]), store, blocks)
    src, spare = Blocks(tmp_ref), [other_ref, tmp_ref]
    for n, (p, t) in reversed(list(enumerate(jumped(targets, branches, levels)))):
        r = 24 + 4 * n
        column = [
            tuple(mid_ref[r + 2 * i + c : r + 2 * i + c + 1, :] for c in range(2)) for i in range(2)
        ]
        dst = Whole(out_ref) if n == 0 else Blocks(spare[(levels - 1 - n) % 2])
        expand(src, dst, p, t, column, 8 if levels == 3 else 2)
        src = dst


def cost(flops):
    return pl.CostEstimate(flops=flops, bytes_accessed=2_000_000, transcendentals=0)


def local_rows(initial_state):
    return initial_state.reshape(2, -1, LANES).transpose(1, 0, 2).reshape(-1, LANES)


def contracted(levels, count, x, *settings):
    vmem, smem = (pl.BlockSpec(memory_space=m) for m in (pltpu.VMEM, pltpu.SMEM))
    tmp = pltpu.VMEM((MID, LANES, 2 * LANES), f32)
    out = pltpu.VMEM((x.shape[0] >> levels, LANES), f32)
    return pl.pallas_call(
        functools.partial(contract_kernel, levels=levels, count=count),
        out_shape=(out, jax.ShapeDtypeStruct((1,), jnp.int32)) if count else out,
        in_specs=[vmem, vmem, smem, smem, smem],
        out_specs=(vmem, smem) if count else vmem,
        scratch_shapes=[tmp] * (levels - 1),
        compiler_params=pltpu.CompilerParams(vmem_limit_bytes=24 << 20),
        cost_estimate=cost(20_000_000),
        name=f"contract_{levels}",
    )(x, *settings)


def program(levels, ready, initial_state, gate_angles, damp_qubits, kraus_branch, damping):
    devices = lax.axis_size(AXES)
    local = initial_state.shape[1]
    whole = float(local * devices)
    rows = local * 2 // LANES
    blocks = MID >> levels
    vmem = pl.BlockSpec(memory_space=pltpu.VMEM)
    smem = pl.BlockSpec(memory_space=pltpu.SMEM)
    big = pltpu.VMEM((2, 256, 256), bf16)
    tmp = pltpu.VMEM((MID, LANES, 2 * LANES), f32)
    near = functools.partial(pltpu.with_memory_space_constraint, memory_space=pltpu.VMEM)
    params = pltpu.CompilerParams(vmem_limit_bytes=24 << 20)
    x = local_rows(initial_state)
    settings = (gate_angles.transpose(1, 0, 2), damp_qubits, kraus_branch, damping)
    table = pltpu.VMEM((2, 256, 256), bf16)
    in_specs = [vmem, vmem, smem, smem, smem]
    sent = x
    if levels:
        sent = ready if levels == 3 else contracted(levels, False, near(x), *settings)
    sent = sent.reshape((devices, 1, 2 * blocks * LANES) if levels > 1 else (devices, 2 * blocks, LANES))
    swapped = lax.all_to_all(sent, AXES, split_axis=0, concat_axis=0, tiled=True)
    unroll = 4 if levels == 3 else 1
    g, sums = pl.pallas_call(
        functools.partial(prep_kernel, unroll=unroll),
        out_shape=(big, pltpu.VMEM((8, LANES), f32)),
        in_specs=[pl.BlockSpec(memory_space=pl.ANY)] + in_specs[1:],
        out_specs=(vmem,) * 2,
        scratch_shapes=[tmp, pltpu.VMEM((56, LANES), f32), table, table,
                        pltpu.VMEM((MID, LANES, LANES), f32), pltpu.VMEM((LANES, LANES), f32),
                        pltpu.VMEM((rows, LANES), f32), pltpu.SemaphoreType.DMA],
        compiler_params=params,
        cost_estimate=cost(2_000_000_000),
        name=f"prep_{levels}",
    )(x, *settings)
    mixed, token = pl.pallas_call(
        functools.partial(global_kernel, blocks=blocks),
        out_shape=(pltpu.VMEM((devices * (2 * blocks + 1), LANES), f32), pltpu.VMEM((8, LANES), f32)),
        in_specs=[vmem] * 3,
        out_specs=(vmem,) * 2,
        compiler_params=params,
        cost_estimate=cost(400_000_000 >> levels),
        name=f"global_gates_{levels}",
    )(near(swapped.reshape(rows >> levels, LANES)), near(g), near(sums))
    back = lax.all_to_all(
        mixed.reshape(devices, 1, (2 * blocks + 1) * LANES), AXES, split_axis=0, concat_axis=0, tiled=True
    )
    low, top, mid = pl.pallas_call(
        functools.partial(tables_kernel, levels=levels, unroll=2),
        out_shape=(big, big, pltpu.VMEM((40, LANES), f32)),
        in_specs=in_specs,
        out_specs=(vmem,) * 3,
        scratch_shapes=[pltpu.VMEM((56, LANES), f32)],
        compiler_params=params,
        cost_estimate=cost(1_000_000_000),
        name=f"tables_{levels}",
    )(near(token), *settings)
    out, weights = pl.pallas_call(
        functools.partial(final_kernel, levels=levels, whole=whole),
        out_shape=(jax.ShapeDtypeStruct((rows, LANES), f32),
                   jax.ShapeDtypeStruct(damp_qubits.shape, f32)),
        in_specs=[vmem] * 4 + [smem] * 2,
        out_specs=(vmem, vmem),
        scratch_shapes=[tmp, tmp],
        compiler_params=params,
        cost_estimate=cost(800_000_000),
        name=f"local_gates_{levels}",
    )(near(back.reshape(devices * (2 * blocks + 1), LANES)), near(low), near(top), near(mid),
      damp_qubits, kraus_branch)
    out = out.reshape(rows // 2, 2, LANES).transpose(1, 0, 2).reshape(2, local)
    return out, weights


def on_device(*args):
    initial_state, gate_angles, *rest = args
    ready, levels = contracted(
        3, True, local_rows(initial_state), gate_angles.transpose(1, 0, 2), *rest
    )
    return lax.switch(levels[0], [functools.partial(program, n) for n in range(4)], ready, *args)


def solution(mesh):
    return jax.shard_map(
        on_device,
        mesh=mesh,
        in_specs=(P(None, AXES), P(), P(), P(), P()),
        out_specs=(P(None, AXES), P()),
        check_vma=False,
    )
```

```python
import functools

import jax
import jax.numpy as jnp
from jax import lax
from jax.experimental import pallas as pl
from jax.experimental.pallas import tpu as pltpu
from jax.sharding import PartitionSpec as P

AXES = ("hi", "lo")
EPS = 1e-6
LANES = 128
ROWS = 16
MID = 8
f32 = jnp.float32
bf16 = jnp.bfloat16


def split(x):
    hi = x.astype(bf16)
    return hi, (x - hi.astype(f32)).astype(bf16)


def dot3(a, b):
    (ah, al), (bh, bl) = a, b
    return jnp.dot(
        jnp.concatenate([ah, ah, al], 1),
        jnp.concatenate([bh, bl, bh], 0),
        preferred_element_type=f32,
    )


def cmul(a, b):
    return a[0] * b[0] - a[1] * b[1], a[0] * b[1] + a[1] * b[0]


def matmul2(a, b):
    out = {}
    for i in range(2):
        for j in range(2):
            p, q = cmul(a[i, 0], b[0, j]), cmul(a[i, 1], b[1, j])
            out[i, j] = (p[0] + q[0], p[1] + q[1])
    return out


def scale2(k, u):
    k00, k01, k11 = k
    out = {}
    for j in range(2):
        out[0, j] = tuple(k00 * u[0, j][c] + k01 * u[1, j][c] for c in range(2))
        out[1, j] = tuple(k11 * u[1, j][c] for c in range(2))
    return out


def gates(angles_ref):
    a, b, c = (angles_ref[k] for k in range(3))
    half = jnp.concatenate([b, a + c, a - c], 0) * 0.5
    cosine, sine = jnp.cos(half), jnp.sin(half)
    out = []
    for layer in range(2):
        co, cs, cd = (cosine[2 * k + layer : 2 * k + layer + 1] for k in range(3))
        si, ss, sd = (sine[2 * k + layer : 2 * k + layer + 1] for k in range(3))
        out.append({
            (0, 0): (cs * co, -ss * co),
            (0, 1): (-cd * si, sd * si),
            (1, 0): (cd * si, sd * si),
            (1, 1): (cs * co, ss * co),
        })
    return out


def tables(angles_ref, targets, branches, rates):
    qubits = angles_ref.shape[2]
    lane = lax.broadcasted_iota(jnp.int32, (1, qubits), 1)
    one, zero = jnp.ones((1, qubits), f32), jnp.zeros((1, qubits), f32)
    u = gates(angles_ref)
    krauses, first = [], zero > 1.0
    for layer in range(2):
        k00, k01, k11 = one, zero, one
        for slot in range(4):
            here = lane == targets[layer, slot]
            jump = branches[layer, slot] == 1
            g = jnp.full((1, qubits), rates[layer, slot], f32)
            k00 = jnp.where(here, jnp.where(jump, 0.0, 1.0), k00)
            k01 = jnp.where(here, jnp.where(jump, jnp.sqrt(g), 0.0), k01)
            k11 = jnp.where(here, jnp.where(jump, 0.0, jnp.sqrt(1.0 - g)), k11)
            if layer == 0:
                first = jnp.logical_or(first, here)
        krauses.append((k00, k01, k11))
    both = matmul2(u[1], u[0])
    v = {
        ij: tuple(jnp.where(first, u[0][ij][c], both[ij][c]) for c in range(2))
        for ij in both
    }
    w = scale2(krauses[0], u[0])
    m = scale2(krauses[1], matmul2(u[1], w))
    into = [tuple(jnp.where(first, w[0, j][c], m[0, j][c]) for c in range(2)) for j in range(2)]
    rest = ((one, zero), (zero, zero))
    out = [tuple(jnp.where(first, u[1][i, 0][c], rest[i][c]) for c in range(2)) for i in range(2)]
    return v, m, into, out


def jumped(targets, branches, levels):
    chosen, count = [jnp.int32(-1)] * levels, jnp.int32(0)
    for layer in range(2):
        for slot in range(4):
            jump = branches[layer, slot] == 1
            for n in range(levels):
                chosen[n] = jnp.where(jnp.logical_and(jump, count == n), targets[layer, slot], chosen[n])
            count = count + jnp.where(jump, 1, 0)
    places = [16 - n for n in range(levels)]
    taken, free = {}, jnp.int32(0)
    for p in places:
        hit = [t == p for t in chosen]
        taken[p] = functools.reduce(jnp.logical_or, hit)
    result, free = [], jnp.int32(0)
    for p in places:
        other, rank = jnp.int32(-1), jnp.int32(0)
        for t in chosen:
            outside = t < 17 - levels
            other = jnp.where(jnp.logical_and(outside, rank == free), t, other)
            rank = rank + jnp.where(outside, 1, 0)
        result.append((p, jnp.where(taken[p], p, other)))
        free = free + jnp.where(taken[p], 0, 1)
    return result


def at_qubit(rows, t):
    lane = lax.broadcasted_iota(jnp.int32, rows[0][0].shape, 1)
    return [
        tuple(
            jnp.broadcast_to(jnp.sum(jnp.where(lane == t, r[c], 0.0), axis=1, keepdims=True), (1, LANES))
            for c in range(2)
        )
        for r in rows
    ]


def moved(m, places):
    lane = lax.broadcasted_iota(jnp.int32, m[0, 0][0].shape, 1)
    out = dict(m)
    for p, t in places:
        here = jnp.logical_and(lane == t, t != p)
        for ij in out:
            out[ij] = tuple(jnp.where(here, m[ij][c][:, p : p + 1], out[ij][c]) for c in range(2))
    return out


def middle_index(m, t, beta):
    bit = jnp.left_shift(jnp.int32(1), t - 14)
    clear = jnp.bitwise_and(m, jnp.bitwise_not(bit))
    return clear + (bit if beta else 0)


def part(c):
    return slice(c * LANES, (c + 1) * LANES)


def two(a, b, x, y):
    p, q = cmul(a, x), cmul(b, y)
    return p[0] + q[0], p[1] + q[1]


class Whole:
    def __init__(self, ref):
        self.ref = ref

    def rows(self, block, tile, c):
        return pl.ds(block * 256 + tile * 16 + c, 8, stride=2)

    def get(self, block, tile, c):
        return self.ref[self.rows(block, tile, c), :]

    def put(self, block, tile, c, value):
        self.ref[self.rows(block, tile, c), :] = value


class Sent(Whole):
    def __init__(self, ref, blocks):
        self.ref, self.blocks = ref, blocks

    def rows(self, block, tile, c):
        return pl.ds(tile * 16 * self.blocks + 2 * block + c, 8, stride=2 * self.blocks)


class Blocks:
    def __init__(self, ref):
        self.ref = ref

    def get(self, block, tile, c):
        return self.ref[block, pl.ds(pl.multiple_of(tile * 8, 8), 8), part(c)]

    def put(self, block, tile, c, value):
        self.ref[block, pl.ds(pl.multiple_of(tile * 8, 8), 8), part(c)] = value


def cases(t, body):
    @pl.when(t < 7)
    def _():
        body("lane", jnp.maximum(t, 0))

    @pl.when(jnp.logical_and(t >= 7, t < 10))
    def _():
        body("row", t - 7)

    @pl.when(jnp.logical_and(t >= 10, t < 14))
    def _():
        body("tile", t - 10)

    @pl.when(t >= 14)
    def _():
        body("middle", t - 14)


def over_tiles(body, unroll):
    def step(i, _):
        body(i)
        return 0

    lax.fori_loop(0, LANES // 8, step, 0, unroll=unroll)


def low_mask(axis, bit):
    index = lax.broadcasted_iota(jnp.int32, (8, LANES), axis)
    return jnp.bitwise_and(index, jnp.left_shift(jnp.int32(1), bit)) == 0


def contract(src, dst, p, t, row, unroll):
    half = 1 << (p - 14)

    def run(kind, bit):
        size = jnp.left_shift(jnp.int32(1), bit)
        axis = 1 if kind == "lane" else 0
        low = low_mask(axis, bit)
        length = LANES if kind == "lane" else 8

        def body(i):
            if kind == "tile":
                up = jnp.bitwise_and(i, size) != 0
                zero, one = jnp.bitwise_and(i, jnp.bitwise_not(size)), jnp.bitwise_or(i, size)
            for m in range(half):
                if kind == "middle":
                    shared = jnp.bitwise_and(jnp.right_shift(m, bit), 1) * half
                    k = [
                        jnp.where(t == p, m + beta * half, middle_index(m, t, beta) + shared)
                        for beta in range(2)
                    ]
                    u, w = ([src.get(n, i, c) for c in range(2)] for n in k)
                elif kind == "tile":
                    k = jnp.where(up, m + half, m)
                    u, w = ([src.get(k, at, c) for c in range(2)] for at in (zero, one))
                else:
                    u, w = [], []
                    for c in range(2):
                        a, b = src.get(m, i, c), src.get(m + half, i, c)
                        u.append(jnp.where(low, a, pltpu.roll(b, size, axis)))
                        w.append(jnp.where(low, pltpu.roll(a, length - size, axis), b))
                for c, value in enumerate(two(row[0], row[1], u, w)):
                    dst.put(m, i, c, value)

        over_tiles(body, unroll)

    cases(t, run)


def expand(src, dst, p, t, column, unroll):
    half = 1 << (p - 14)

    def run(kind, bit):
        size = jnp.left_shift(jnp.int32(1), bit)
        axis = 1 if kind == "lane" else 0
        low = low_mask(axis, bit)
        length = LANES if kind == "lane" else 8
        if kind in ("lane", "row"):
            e = tuple(jnp.where(low, column[0][c], column[1][c]) for c in range(2))

        def body(i):
            if kind == "tile":
                up = jnp.bitwise_and(i, size) != 0
                at = (jnp.bitwise_and(i, jnp.bitwise_not(size)), jnp.bitwise_or(i, size))
                ei = tuple(jnp.where(up, column[1][c], column[0][c]) for c in range(2))
            for m in range(half):
                if kind == "middle":
                    shared = jnp.bitwise_and(jnp.right_shift(m, bit), 1) * half
                    y = [src.get(m, i, c) for c in range(2)]
                    made = [
                        (jnp.where(t == p, m + beta * half, middle_index(m, t, beta) + shared), cmul(column[beta], y))
                        for beta in range(2)
                    ]
                elif kind == "tile":
                    made = [
                        (m + s * half, cmul(ei, [src.get(m, at[s], c) for c in range(2)]))
                        for s in range(2)
                    ]
                else:
                    y = [src.get(m, i, c) for c in range(2)]
                    s0 = [jnp.where(low, v, pltpu.roll(v, size, axis)) for v in y]
                    s1 = [jnp.where(low, pltpu.roll(v, length - size, axis), v) for v in y]
                    made = [(m, cmul(e, s0)), (m + half, cmul(e, s1))]
                for k, value in made:
                    for c in range(2):
                        dst.put(k, i, c, value[c])

        over_tiles(body, unroll)

    cases(t, run)


def entry(table, ij, c, qubit):
    return table[ij][c][:, qubit : qubit + 1]


def store_kron(ref, rows_ref, table, start, right, unroll):
    names = ((0, 0), (0, 1), (1, 0), (1, 1))
    for j in range(7):
        for n, ij in enumerate(names):
            for c in range(2):
                r = 8 * j + 2 * n + c
                rows_ref[r : r + 1, :] = jnp.broadcast_to(entry(table, ij, c, start + j), (1, LANES))
    step = 16

    def row(j, n, c):
        r = 8 * j + 2 * n + c
        return rows_ref[r : r + 1, :]

    rows = lax.broadcasted_iota(jnp.int32, (step, LANES), 0)
    cols = lax.broadcasted_iota(jnp.int32, (step, LANES), 1)
    if right:
        rows, cols = cols, rows
    shared = None
    for j in range(4):
        rb = jnp.bitwise_and(rows, 1 << j) == 0
        cb = jnp.bitwise_and(cols, 1 << j) == 0
        e = tuple(
            jnp.where(rb, jnp.where(cb, row(j, 0, c), row(j, 1, c)), jnp.where(cb, row(j, 2, c), row(j, 3, c)))
            for c in range(2)
        )
        shared = e if shared is None else cmul(shared, e)
    lane = lax.broadcasted_iota(jnp.int32, (1, LANES), 1)

    def body(i, _):
        at = pl.multiple_of(i * step, step)
        own = None
        for j in range(4, 7):
            zero = jnp.bitwise_and(jnp.right_shift(i, j - 4), 1) == 0
            first = jnp.bitwise_and(lane, 1 << j) == 0
            e = []
            for c in range(2):
                w = [row(j, n, c) for n in range(4)]
                a = jnp.where(zero, w[0], w[1] if right else w[2])
                b = jnp.where(zero, w[2] if right else w[1], w[3])
                e.append(jnp.where(first, a, b))
            own = tuple(e) if own is None else cmul(own, e)
        acc = cmul(shared, own)
        for n, (re, im) in enumerate(zip(split(acc[0]), split(acc[1]))):
            here, below = pl.ds(at, step), pl.ds(at + LANES, step)
            ref[n, here, :LANES] = re
            ref[n, below, LANES:] = re
            ref[n, here, LANES:] = im if right else -im
            ref[n, below, :LANES] = -im if right else im
        return 0

    lax.fori_loop(0, LANES // step, body, 0, unroll=unroll)


def mid_mix(load, store, coef, bits, blocks):
    x = [load(q) for q in range(blocks)]
    for j in bits:
        for q in range(blocks):
            if q >> j & 1:
                continue
            p = q | 1 << j
            x0, x1 = x[q], x[p]
            new = []
            for i in range(2):
                a, b = cmul(coef(j, i, 0), x0), cmul(coef(j, i, 1), x1)
                new.append((a[0] + b[0], a[1] + b[1]))
            x[q], x[p] = new
    for q in range(blocks):
        store(q, x[q])


def strided(start, stride):
    return pl.ds(start, LANES, stride=stride)


def right_stage(load, weights, tmp_ref, blocks=MID):
    for q in range(blocks):
        x = jnp.concatenate([load(q, c) for c in range(2)], 1)
        tmp_ref[q] = dot3(split(x), weights)


def left_stage(load, weights, store, blocks=MID):
    for q in range(0, blocks, 2):
        group = range(q, min(q + 2, blocks))
        ys = left_group(weights, [tuple(load(p, c) for c in range(2)) for p in group])
        for p, y in zip(group, ys):
            for c in range(2):
                store(p, c, y[c])


def mid_stage(tmp_ref, coef, bits, blocks, unroll):
    def body(i, _):
        at = pl.ds(pl.multiple_of(i * 8, 8), 8)

        def load(q):
            return tmp_ref[q, at, :LANES], tmp_ref[q, at, LANES:]

        def store(q, value):
            tmp_ref[q, at, :LANES], tmp_ref[q, at, LANES:] = value

        mid_mix(load, store, coef, bits, blocks)
        return 0

    lax.fori_loop(0, LANES // 8, body, 0, unroll=unroll)


def left_group(weights, pairs):
    x = jnp.concatenate([jnp.concatenate([a[c] for a in pairs], 1) for c in range(2)], 0)
    y = dot3(weights, split(x))
    return [
        tuple(y[c * LANES : (c + 1) * LANES, p * LANES : (p + 1) * LANES] for c in range(2))
        for p in range(len(pairs))
    ]


def level_sums(squares, mixed_ref, targets, branches, rates, layer):
    lane = lax.broadcasted_iota(jnp.int32, (LANES, LANES), 1)
    row = lax.broadcasted_iota(jnp.int32, (LANES, LANES), 0)
    weight = jnp.ones((LANES, LANES), f32)
    wq = [jnp.float32(1.0)] * MID
    out = []

    def total(v):
        return jnp.sum(jnp.sum(v, axis=0, keepdims=True), axis=1, keepdims=True)

    def mix(wq):
        mixed = wq[0] * squares[0]
        for q in range(1, MID):
            mixed = mixed + wq[q] * squares[q]
        mixed_ref[...] = mixed

    for slot in range(5):
        if slot == 0:
            mix(wq)
        else:

            @pl.when(mid)
            def _(now=tuple(wq)):
                mix(now)

        out.append(total(mixed_ref[...] * weight))
        if slot == 4:
            break
        t = targets[layer, slot]
        g = rates[layer, slot]
        jump = branches[layer, slot] == 1
        f0 = jnp.where(jump, 0.0, 1.0)
        f1 = jnp.where(jump, g, 1.0 - g)
        low, mid = t < 7, t >= 14
        index = jnp.where(low, lane, row)
        shift = jnp.where(low, t, jnp.clip(t - 7, 0, 6))
        bit = jnp.bitwise_and(jnp.right_shift(index, shift), 1)
        factor = jnp.where(bit == 1, f1, f0)
        weight = weight * jnp.where(mid, jnp.ones_like(factor), factor)
        tm = jnp.where(mid, t - 14, 0)
        wq = [
            w * jnp.where(mid, jnp.where(jnp.bitwise_and(jnp.right_shift(q, tm), 1) == 1, f1, f0), 1.0)
            for q, w in enumerate(wq)
        ]
    return out, weight, wq


def prep_kernel(x_hbm, angles_ref, targets, branches, rates, g_ref, sums_ref,
                tmp_ref, rows_ref, low_v_ref, top_v_ref, squares_ref, mixed_ref,
                x_ref, sem, *, unroll):
    copy = pltpu.make_async_copy(x_hbm, x_ref, sem)
    copy.start()
    v, m, _, _ = tables(angles_ref, targets, branches, rates)
    store_kron(g_ref, rows_ref, m, 17, False, min(unroll, 8))
    store_kron(low_v_ref, rows_ref, v, 0, True, min(unroll, 8))
    store_kron(top_v_ref, rows_ref, v, 7, False, min(unroll, 8))
    v_low, v_top = ((r[0], r[1]) for r in (low_v_ref, top_v_ref))
    copy.wait()
    right_stage(lambda q, c: x_ref[strided(q * 256 + c, 2), :], v_low, tmp_ref)
    v_mid = {
        (j, i, k, c): jnp.broadcast_to(entry(v, (i, k), c, 14 + j), (8, LANES))
        for j in range(3) for i in range(2) for k in range(2) for c in range(2)
    }
    for bit in range(3):
        hits = [targets[layer, slot] == 14 + bit for layer in range(2) for slot in range(4)]

        @pl.when(functools.reduce(jnp.logical_or, hits))
        def _(bit=bit):
            mid_stage(
                tmp_ref, lambda j, i, k: (v_mid[j, i, k, 0], v_mid[j, i, k, 1]), [bit], MID, unroll
            )


    def keep(p, c, value):
        tmp_ref[p, :, part(c)] = value

    left_stage(lambda p, c: tmp_ref[p, :, part(c)], v_top, keep)
    for q in range(MID):
        re, im = (tmp_ref[q, :, part(c)] for c in range(2))
        squares_ref[q] = re * re + im * im
    first, weight, wq = level_sums(squares_ref, mixed_ref, targets, branches, rates, 0)
    kept = first[4]
    alpha = jnp.where(kept > 0.0, lax.rsqrt(jnp.maximum(kept, 1e-37)), 0.0)
    root = jnp.sqrt(weight)
    for q in range(MID):
        r = root * jnp.sqrt(jnp.full((1, LANES), wq[q], f32)) * alpha
        re, im = (tmp_ref[q, :, part(c)] * r for c in range(2))
        squares_ref[q] = re * re + im * im
    second, _, _ = level_sums(squares_ref, mixed_ref, targets, branches, rates, 1)
    base = jnp.where(second[0] > 0.0, second[0], 1.0)
    values = first + [s / base for s in second[1:]]
    lane = lax.broadcasted_iota(jnp.int32, (8, LANES), 1)
    packed = jnp.zeros((8, LANES), f32)
    for k, s in enumerate(values):
        packed = jnp.where(lane == k, s, packed)
    sums_ref[...] = packed


def tables_kernel(after_ref, angles_ref, targets, branches, rates, low_ref, top_ref, mid_ref, rows_ref, *, levels, unroll):
    _, m, _, out = tables(angles_ref, targets, branches, rates)
    places = jumped(targets, branches, levels)
    for n, (_, t) in enumerate(places):
        e = at_qubit(out, t)
        for i in range(2):
            for c in range(2):
                r = 24 + 4 * n + 2 * i + c
                mid_ref[r : r + 1, :] = e[i][c]
    m = moved(m, places)
    store_kron(low_ref, rows_ref, m, 0, True, unroll)
    store_kron(top_ref, rows_ref, m, 7, False, unroll)
    for j in range(3):
        for i in range(2):
            for k in range(2):
                for c in range(2):
                    r = ((j * 2 + i) * 2 + k) * 2 + c
                    mid_ref[r : r + 1, :] = jnp.broadcast_to(
                        entry(m, (i, k), c, 14 + j), (1, LANES)
                    )


def contract_kernel(x_ref, angles_ref, targets, branches, rates, out_ref, *refs, levels, count):
    spare = list(refs)
    if count:
        count_ref = spare.pop(0)
        jumps = jnp.int32(0)
        for layer in range(2):
            for slot in range(4):
                jumps = jumps + jnp.where(branches[layer, slot] == 1, 1, 0)
        count_ref[0] = jnp.minimum(jumps, levels)
    _, _, into, _ = tables(angles_ref, targets, branches, rates)
    places = jumped(targets, branches, levels)
    rows = [at_qubit(into, t) for _, t in places]
    src = Whole(x_ref)
    for n, (p, t) in enumerate(places):
        dst = Sent(out_ref, MID >> levels) if n == levels - 1 else Blocks(spare[n])
        contract(src, dst, p, t, rows[n], 8 if count else 4)
        src = dst


def global_kernel(x_ref, g_ref, sums_ref, out_ref, token_ref, *, blocks):
    token_ref[...] = sums_ref[...]
    stride = 2 * blocks + 1

    def store(p, c, value):
        out_ref[strided(2 * p + c, stride), :] = value

    left_stage(
        lambda p, c: x_ref[strided(2 * p + c, 2 * blocks), :], (g_ref[0], g_ref[1]), store, blocks
    )
    out_ref[strided(2 * blocks, stride), :] = jnp.broadcast_to(
        sums_ref[0:1, :], (LANES, LANES)
    )


def final_kernel(x_ref, low_ref, top_ref, mid_ref, targets, branches,
                 out_ref, weights_ref, tmp_ref, other_ref, *, levels, whole):
    blocks = MID >> levels
    stride = 2 * blocks + 1
    parts = x_ref[strided(2 * blocks, stride), :]
    totals = jnp.sum(parts, axis=0, keepdims=True)
    kept = parts[:, 4:5]
    kept_total = jnp.maximum(totals[:, 4:5], 1e-37)
    ratios = jnp.sum(parts * (kept / kept_total), axis=0, keepdims=True)
    lane = lax.broadcasted_iota(jnp.int32, (1, LANES), 1)
    row = jnp.zeros((1, LANES), f32)
    factors = []
    mean = [totals[:, k : k + 1] / whole for k in range(5)]
    for layer in range(2):
        factor = jnp.ones((1, 1), f32)
        for slot in range(4):
            before = mean[slot] * factor * factor
            after = mean[slot + 1] * factor * factor
            row = jnp.where(lane == layer * 4 + slot, after / before, row)
            factor = factor * lax.rsqrt(after + EPS)
        factors.append(factor)
        if layer == 0:
            start = mean[4] * factor * factor
            mean = [start] + [start * ratios[:, 5 + k : 6 + k] for k in range(4)]
    weights_ref[0:1, :] = row[:, 0:4]
    weights_ref[1:2, :] = row[:, 4:8]

    def load(q, c):
        if levels:
            return x_ref[strided(2 * q + c, stride), :]
        return jnp.concatenate(
            [x_ref[pl.ds((q * 16 + k) * stride + c, 8, stride=2), :] for k in range(16)], 0
        )

    right_stage(load, (low_ref[0], low_ref[1]), tmp_ref, blocks)

    def coef(j, i, k):
        r = ((j * 2 + i) * 2 + k) * 2
        return mid_ref[r : r + 1, :], mid_ref[r + 1 : r + 2, :]

    if levels < 3:
        mid_stage(tmp_ref, coef, range(3 - levels), blocks, 2)

    def store(q, c, value):
        value = value * factors[0] * factors[1]
        if levels:
            tmp_ref[q, :, part(c)] = value
        else:
            out_ref[strided(q * 256 + c, 2), :] = value

    left_stage(lambda q, c: tmp_ref[q, :, part(c)], (top_ref[0], top_ref[1]), store, blocks)
    src, spare = Blocks(tmp_ref), [other_ref, tmp_ref]
    for n, (p, t) in reversed(list(enumerate(jumped(targets, branches, levels)))):
        r = 24 + 4 * n
        column = [
            tuple(mid_ref[r + 2 * i + c : r + 2 * i + c + 1, :] for c in range(2)) for i in range(2)
        ]
        dst = Whole(out_ref) if n == 0 else Blocks(spare[(levels - 1 - n) % 2])
        expand(src, dst, p, t, column, 8 if levels == 3 else 4)
        src = dst


def cost(flops):
    return pl.CostEstimate(flops=flops, bytes_accessed=2_000_000, transcendentals=0)


def local_rows(initial_state):
    return initial_state.reshape(2, -1, LANES).transpose(1, 0, 2).reshape(-1, LANES)


def contracted(levels, count, x, *settings):
    vmem, smem = (pl.BlockSpec(memory_space=m) for m in (pltpu.VMEM, pltpu.SMEM))
    tmp = pltpu.VMEM((MID, LANES, 2 * LANES), f32)
    out = pltpu.VMEM((x.shape[0] >> levels, LANES), f32)
    return pl.pallas_call(
        functools.partial(contract_kernel, levels=levels, count=count),
        out_shape=(out, jax.ShapeDtypeStruct((1,), jnp.int32)) if count else out,
        in_specs=[vmem, vmem, smem, smem, smem],
        out_specs=(vmem, smem) if count else vmem,
        scratch_shapes=[tmp] * (levels - 1),
        compiler_params=pltpu.CompilerParams(vmem_limit_bytes=24 << 20),
        cost_estimate=cost(20_000_000),
        name=f"contract_{levels}",
    )(x, *settings)


def program(levels, ready, initial_state, gate_angles, damp_qubits, kraus_branch, damping):
    devices = lax.axis_size(AXES)
    local = initial_state.shape[1]
    whole = float(local * devices)
    rows = local * 2 // LANES
    blocks = MID >> levels
    vmem = pl.BlockSpec(memory_space=pltpu.VMEM)
    smem = pl.BlockSpec(memory_space=pltpu.SMEM)
    big = pltpu.VMEM((2, 256, 256), bf16)
    tmp = pltpu.VMEM((MID, LANES, 2 * LANES), f32)
    near = functools.partial(pltpu.with_memory_space_constraint, memory_space=pltpu.VMEM)
    params = pltpu.CompilerParams(vmem_limit_bytes=24 << 20)
    x = local_rows(initial_state)
    settings = (gate_angles.transpose(1, 0, 2), damp_qubits, kraus_branch, damping)
    table = pltpu.VMEM((2, 256, 256), bf16)
    in_specs = [vmem, vmem, smem, smem, smem]
    sent = x
    if levels:
        sent = ready if levels == 3 else contracted(levels, False, near(x), *settings)
    sent = sent.reshape((devices, 1, 2 * blocks * LANES) if levels > 1 else (devices, 2 * blocks, LANES))
    swapped = lax.all_to_all(sent, AXES, split_axis=0, concat_axis=0, tiled=True)
    unroll = 4 if levels == 3 else 1
    g, sums = pl.pallas_call(
        functools.partial(prep_kernel, unroll=unroll),
        out_shape=(big, pltpu.VMEM((8, LANES), f32)),
        in_specs=[pl.BlockSpec(memory_space=pl.ANY)] + in_specs[1:],
        out_specs=(vmem,) * 2,
        scratch_shapes=[tmp, pltpu.VMEM((56, LANES), f32), table, table,
                        pltpu.VMEM((MID, LANES, LANES), f32), pltpu.VMEM((LANES, LANES), f32),
                        pltpu.VMEM((rows, LANES), f32), pltpu.SemaphoreType.DMA],
        compiler_params=params,
        cost_estimate=cost(2_000_000_000),
        name=f"prep_{levels}",
    )(x, *settings)
    mixed, token = pl.pallas_call(
        functools.partial(global_kernel, blocks=blocks),
        out_shape=(pltpu.VMEM((devices * (2 * blocks + 1), LANES), f32), pltpu.VMEM((8, LANES), f32)),
        in_specs=[vmem] * 3,
        out_specs=(vmem,) * 2,
        compiler_params=params,
        cost_estimate=cost(400_000_000 >> levels),
        name=f"global_gates_{levels}",
    )(near(swapped.reshape(rows >> levels, LANES)), near(g), near(sums))
    back = lax.all_to_all(
        mixed.reshape(devices, 1, (2 * blocks + 1) * LANES), AXES, split_axis=0, concat_axis=0, tiled=True
    )
    low, top, mid = pl.pallas_call(
        functools.partial(tables_kernel, levels=levels, unroll=2),
        out_shape=(big, big, pltpu.VMEM((40, LANES), f32)),
        in_specs=in_specs,
        out_specs=(vmem,) * 3,
        scratch_shapes=[pltpu.VMEM((56, LANES), f32)],
        compiler_params=params,
        cost_estimate=cost(1_000_000_000),
        name=f"tables_{levels}",
    )(near(token), *settings)
    out, weights = pl.pallas_call(
        functools.partial(final_kernel, levels=levels, whole=whole),
        out_shape=(jax.ShapeDtypeStruct((rows, LANES), f32),
                   jax.ShapeDtypeStruct(damp_qubits.shape, f32)),
        in_specs=[vmem] * 4 + [smem] * 2,
        out_specs=(vmem, vmem),
        scratch_shapes=[tmp, tmp],
        compiler_params=params,
        cost_estimate=cost(800_000_000),
        name=f"local_gates_{levels}",
    )(near(back.reshape(devices * (2 * blocks + 1), LANES)), near(low), near(top), near(mid),
      damp_qubits, kraus_branch)
    out = out.reshape(rows // 2, 2, LANES).transpose(1, 0, 2).reshape(2, local)
    return out, weights


def on_device(*args):
    initial_state, gate_angles, *rest = args
    ready, levels = contracted(
        3, True, local_rows(initial_state), gate_angles.transpose(1, 0, 2), *rest
    )
    return lax.switch(levels[0], [functools.partial(program, n) for n in range(4)], ready, *args)


def solution(mesh):
    return jax.shard_map(
        on_device,
        mesh=mesh,
        in_specs=(P(None, AXES), P(), P(), P(), P()),
        out_specs=(P(None, AXES), P()),
        check_vma=False,
    )
```
